256 devices in a mesh: cp: 32 (over y_lo, z, core), tp: 8 (over x, y_hi).
Axes of the slice: x: 4, y: 4 (y_hi: 2, y_lo: 2; y = y_hi * 2 + y_lo), z: 8, core: 2. Of those that a mesh axis runs over, the one named last changes fastest.
Arguments:
- hidden_in: bfloat16 [8192, 5120], P('cp', 'tp'), may hold values from -6 to 6
- norm_gain: float32 [5120], replicated, may hold values from 0.25 to 1.75
- seq_lengths: int32 [16], replicated, may hold values from 1 to 6144, 8192 in all
- w_query: bfloat16 [5120, 3072], P(None, 'tp'), may hold values from -0.078125 to 0.078125
- b_query: bfloat16 [3072], P('tp'), may hold values from -400 to 400
- w_key: bfloat16 [5120, 1024], P(None, 'tp'), may hold values from -0.078125 to 0.078125
- b_key: bfloat16 [1024], P('tp'), may hold values from -3 to 3
- w_value: bfloat16 [5120, 1024], P(None, 'tp'), may hold values from -0.078125 to 0.078125
- b_value: bfloat16 [1024], P('tp'), may hold values from -3 to 3
- w_out: bfloat16 [3072, 5120], P(None, 'tp'), may hold values from -0.109375 to 0.109375
Outputs:
- mixed: bfloat16 [8192, 5120], P('cp', 'tp')
- k_cache: bfloat16 [8192, 1024], P('cp', 'tp')
- v_cache: bfloat16 [8192, 1024], P('cp', 'tp')
The draws below stay inside these ranges and needn't reach their ends.
Inputs may be any that keep to these rules, and one draw needn't show every extreme that they name: `seq_lengths`: they sum to 8192; the longest is exactly 6144.
All inputs are finite; a program needn't handle non-finite values.
Results may differ from the reference program's by a relative error of at most 0.012.
The reference program's roundings to bfloat16 on the way (of `normed`, `query`, `weights` and `attended`) count: a program that leaves them out, or rounds other values in their place, can miss the bound.
Values may be sent and summed in bfloat16 or wider, within the bound.
A program may use at most 64 MiB of HBM per device.

```python
import math
import jax
import jax.numpy as jnp
import numpy as np
from jax import lax

D = 5120
KVH = 8
HD = 128
QH = 24
SEQS = 16
TOKENS = 8192
MOST = 6144


def draw_b_query(key, part):
    base = jax.random.normal(jax.random.fold_in(key, 11), (QH * HD,), jnp.float32)
    return jnp.clip(0.5 * base, -3.0, 3.0).astype(jnp.bfloat16)


def shard_levels(own_key, extent, shards, least, top_value):
    def one(axis_at, blocks):
        steps = jax.random.uniform(jax.random.fold_in(jax.random.fold_in(own_key, 6), axis_at), (blocks,), jnp.float32, least / len(shards), top_value / len(shards))
        return jnp.repeat(jnp.exp(steps), extent[axis_at] // blocks).reshape((-1,) + (1,) * (len(extent) - axis_at - 1))

    level = one(*shards[0])
    for cut in shards[1:]:
        level = level * one(*cut)
    return level


def length_profile(number_of, total, limit, skew):
    portions = [(1 << 20) // math.isqrt(grade ** skew) + 1 for grade in range(2, number_of + 1)]
    spare, holding = total - limit - (number_of - 1), [1] * (number_of - 1)
    while spare > 0:
        candidates = [i for i in range(number_of - 1) if holding[i] < limit]
        whole, remaining = sum([portions[i] for i in candidates]), spare
        for i in candidates:
            more = min(limit - holding[i], max(1, remaining * portions[i] // whole), spare)
            holding[i] = holding[i] + more
            spare = spare - more
    return np.array([limit] + holding)


def ragged_sizes(rng, number_of, total, bound, slope):
    if number_of == 2:
        one = jax.random.randint(rng, (), max(1, total - bound), min(bound, total - 1) + 1)
        return jnp.stack([one, total - one])
    lengths = jnp.asarray(length_profile(number_of, total, bound, slope), jnp.int32)
    twos = (number_of - 1) // 2
    donor, sink = lengths[1:1 + 2 * twos:2], lengths[2:2 + 2 * twos:2]
    margin = jnp.minimum(donor - 1, bound - sink)
    shifted = jax.random.randint(jax.random.fold_in(rng, 1), (twos,), 0, 1 << 20) % (margin + 1)
    lengths = lengths.at[1:1 + 2 * twos:2].set(donor - shifted).at[2:2 + 2 * twos:2].set(sink + shifted)
    return lengths[jax.random.permutation(jax.random.fold_in(rng, 2), number_of)]


def gaussian(rng, dims, scale, reach, shards=(), kind=jnp.bfloat16):
    values = scale * jax.random.normal(rng, dims, jnp.float32)
    if shards:
        values = values * shard_levels(rng, dims, shards, -0.22, 0.18)
    return jnp.clip(values, -reach, reach).astype(kind)


def setup_inputs(seed: int = 0) -> dict:
    streams_of = jax.random.split(jax.random.key(seed), 11)
    return {
        "hidden_in": gaussian(streams_of[0], (TOKENS, D), 1.0, 6.0, ((0, 32), (1, 8))),
        "norm_gain": jnp.clip(1.0 + 0.15 * jax.random.normal(streams_of[1], (D,), jnp.float32), 0.25, 1.75),
        "seq_lengths": ragged_sizes(streams_of[2], SEQS, TOKENS, MOST, 2).astype(jnp.int32),
        "w_query": gaussian(streams_of[3], (D, QH * HD), D ** -0.5, 0.078125, ((1, 8),)),
        "b_query": draw_b_query(jax.random.fold_in(streams_of[10], 71), 0),
        "w_key": gaussian(streams_of[5], (D, KVH * HD), D ** -0.5, 0.078125, ((1, 8),)),
        "b_key": gaussian(streams_of[6], (KVH * HD,), 0.5, 3.0, ((0, 8),)),
        "w_value": gaussian(streams_of[7], (D, KVH * HD), D ** -0.5, 0.078125, ((1, 8),)),
        "b_value": gaussian(streams_of[8], (KVH * HD,), 0.5, 3.0, ((0, 8),)),
        "w_out": gaussian(streams_of[9], (QH * HD, D), (QH * HD) ** -0.5, 0.109375, ((1, 8),)),
    }


EPS = 1e-06
ROPE_BASE = 1000000.0
NEG = -1e+30

def doc_tables(seq_lengths, positions):
    ends = jnp.cumsum(seq_lengths).astype(jnp.int32)
    starts = (ends - seq_lengths).astype(jnp.int32)
    after = positions[:, None] >= ends[None, :]
    docs = lax.optimization_barrier(jnp.sum(after.astype(jnp.int32), axis=1)).astype(jnp.int32)
    inside = (positions[:, None] >= starts[None, :]) & jnp.logical_not(after)
    offset = lax.optimization_barrier(jnp.sum(jnp.where(inside, starts[None, :], 0), axis=1)).astype(jnp.int32)
    return (docs, (positions - offset).astype(jnp.int32))

def rotate(values, positions):
    half = values.shape[-1] // 2
    freq = ROPE_BASE ** (-jnp.arange(half, dtype=jnp.float32) / half)
    angle = positions.astype(jnp.float32)[:, None] * freq[None, :]
    cosine = jnp.cos(angle)[:, None, :]
    sine = jnp.sin(angle)[:, None, :]
    first = values[..., :half]
    second = values[..., half:]
    return jnp.concatenate([first * cosine - second * sine, second * cosine + first * sine], axis=-1)

def reference(hidden_in, norm_gain, seq_lengths, w_query, b_query, w_key, b_key, w_value, b_value, w_out):
    positions = jnp.arange(TOKENS, dtype=jnp.int32)
    docs, local_pos = doc_tables(seq_lengths, positions)
    widened = hidden_in.astype(jnp.float32)
    normed = (widened * lax.rsqrt(lax.optimization_barrier(jnp.mean(widened * widened, axis=-1, keepdims=True)) + EPS) * norm_gain).astype(jnp.bfloat16)
    query = jnp.dot(normed, w_query, preferred_element_type=jnp.float32) + b_query.astype(jnp.float32)
    query = rotate(query.reshape(TOKENS, QH, HD), local_pos).astype(jnp.bfloat16)
    keys = jnp.dot(normed, w_key, preferred_element_type=jnp.float32) + b_key.astype(jnp.float32)
    keys = rotate(keys.reshape(TOKENS, KVH, HD), local_pos).astype(jnp.bfloat16)
    values = (jnp.dot(normed, w_value, preferred_element_type=jnp.float32) + b_value.astype(jnp.float32)).astype(jnp.bfloat16)
    value_heads = values.reshape(TOKENS, KVH, HD)
    group = QH // KVH
    grouped = query.reshape(TOKENS, KVH, group, HD)
    block = math.gcd(512, TOKENS)
    window = min(TOKENS, MOST + block)
    scale = HD ** (-0.5)

    def one_block(index):
        q_start = (index * block).astype(jnp.int32)
        k_start = jnp.clip(q_start - MOST, 0, TOKENS - window).astype(jnp.int32)
        q_rows = lax.dynamic_slice_in_dim(grouped, q_start, block, 0).astype(jnp.float32)
        k_rows = lax.dynamic_slice_in_dim(keys, k_start, window, 0).astype(jnp.float32)
        v_rows = lax.dynamic_slice_in_dim(value_heads, k_start, window, 0).astype(jnp.float32)
        q_pos = q_start + jnp.arange(block, dtype=jnp.int32)
        k_pos = k_start + jnp.arange(window, dtype=jnp.int32)
        q_doc = lax.dynamic_slice_in_dim(docs, q_start, block, 0)
        k_doc = lax.dynamic_slice_in_dim(docs, k_start, window, 0)
        allowed = (k_pos[None, :] <= q_pos[:, None]) & (k_doc[None, :] == q_doc[:, None])
        scores = jnp.einsum('qhgd,khd->hgqk', q_rows, k_rows) * scale
        highest = lax.optimization_barrier(jnp.max(jnp.where(allowed, scores, NEG), axis=-1, keepdims=True))
        weights = jnp.exp(jnp.where(allowed, scores - highest, NEG))
        totals = lax.optimization_barrier(jnp.sum(weights, axis=-1))
        rounded = lax.optimization_barrier(weights.astype(jnp.bfloat16))
        summed = jnp.einsum('hgqk,khd->qhgd', rounded.astype(jnp.float32), v_rows)
        result = summed / jnp.transpose(totals, (2, 0, 1))[..., None]
        return result.astype(jnp.bfloat16).reshape(block, QH * HD)
    attended = lax.map(one_block, jnp.arange(TOKENS // block, dtype=jnp.int32)).reshape(TOKENS, QH * HD)
    projected = jnp.dot(attended, w_out, preferred_element_type=jnp.float32)
    mixed = (widened + projected).astype(jnp.bfloat16)
    return (mixed, keys.reshape(TOKENS, KVH * HD), values)
```

```python
import functools

import jax
import jax.numpy as jnp
from jax import lax
from jax.experimental import pallas as pl
from jax.experimental.pallas import tpu as pltpu
from jax.sharding import PartitionSpec as P

HD = 128
EPS = 1e-06
ROPE_BASE = 1000000.0
NEG = -1e30
MESH = pl.DeviceIdType.MESH
BF = jnp.bfloat16
F32 = jnp.float32
LEFT, RIGHT, OPP, PART, PLEFT, PRIGHT, POPP = 1, 2, 3, 4, 5, 6, 7
SENDS = 80


def kernel(
    hid, gain, seq, wq, bq, wk, bk, wv, bv, wo, freq,
    mixed, kout, vout,
    G, N, W, Wo, Kb, Vb, AT, Q, M, L, ACC, COS, SIN, START, SS, OACC,
    lsem, a_send, a_recv, c_send, c_recv, kv_send, kv_recv,
):
    T = hid.shape[0]
    D1 = hid.shape[1]
    H1 = wo.shape[0] // 8
    NH = H1 // HD
    half = T // 2
    cp = lax.axis_index("cp")
    tp = lax.axis_index("tp")
    y = lax.div(cp, 16)
    z = lax.div(lax.rem(cp, 16), 2)
    k = lax.rem(cp, 2)
    x = lax.div(tp, 2)
    yh = lax.rem(tp, 2)
    xl = lax.rem(x + 3, 4)
    xr = lax.rem(x + 1, 4)
    xo = lax.rem(x + 2, 4)
    right = (cp, 2 * xr + yh)
    left = (cp, 2 * xl + yh)
    partner = (cp, 2 * x + 1 - yh)
    zplus = (y * 16 + lax.rem(z + 1, 8) * 2 + k, tp)
    zminus = (y * 16 + lax.rem(z + 7, 8) * 2 + k, tp)
    ypart = ((1 - y) * 16 + z * 2 + k, tp)
    sib = (y * 16 + z * 2 + 1 - k, tp)

    own_cols = pl.ds(pl.multiple_of(tp * D1, 128), D1)
    load_hid = pltpu.make_async_copy(hid, G.at[:, own_cols], lsem.at[0])
    load_hid.start()
    loads = [
        pltpu.make_async_copy(wk, W.at[:, pl.ds(H1, HD)], lsem.at[1]),
        pltpu.make_async_copy(wv, W.at[:, pl.ds(H1 + HD, HD)], lsem.at[2]),
        pltpu.make_async_copy(wq, W.at[:, pl.ds(0, H1)], lsem.at[3]),
        pltpu.make_async_copy(wo, Wo, lsem.at[4]),
    ]

    barrier = pltpu.get_barrier_semaphore()
    for dev in (right, left, partner, zplus, zminus, ypart, sib):
        pl.semaphore_signal(barrier, inc=1, device_id=dev, device_id_type=MESH)
    for c in loads:
        c.start()
    pl.semaphore_wait(barrier, 7)
    load_hid.wait()

    tps = {
        0: 2 * x + yh, LEFT: 2 * xl + yh, RIGHT: 2 * xr + yh, OPP: 2 * xo + yh,
        PART: 2 * x + 1 - yh, PLEFT: 2 * xl + 1 - yh, PRIGHT: 2 * xr + 1 - yh, POPP: 2 * xo + 1 - yh,
    }

    class Gather:
        def __init__(self, buf, width, ssem, rsem):
            self.buf, self.width, self.ssem, self.rsem = buf, width, ssem, rsem
            self.sent = []

        def ref(self, slot, h):
            cols = pl.ds(pl.multiple_of(tps[slot] * self.width, 128), self.width)
            return self.buf.at[pl.ds(h * half, half), cols]

        def send(self, slot, h, dev, dst_slot):
            r = self.ref(slot, h)
            c = pltpu.make_async_remote_copy(
                src_ref=r, dst_ref=r, send_sem=self.ssem.at[len(self.sent)],
                recv_sem=self.rsem.at[dst_slot * 2 + h], device_id=dev, device_id_type=MESH,
            )
            c.start()
            self.sent.append(c)

        def wait(self, slot, h):
            r = self.ref(slot, h)
            pltpu.make_async_remote_copy(
                src_ref=r, dst_ref=r, send_sem=self.ssem.at[0],
                recv_sem=self.rsem.at[slot * 2 + h], device_id=right, device_id_type=MESH,
            ).wait_recv()

        def start(self):
            self.send(0, 0, right, LEFT)
            self.send(0, 1, left, RIGHT)
            self.send(0, 0, partner, PART)
            self.send(0, 1, right, LEFT)
            self.send(0, 0, left, RIGHT)
            self.send(0, 1, partner, PART)

        def run(self, hooks):
            self.wait(LEFT, 0)
            self.send(LEFT, 0, right, OPP)
            self.wait(RIGHT, 1)
            self.send(RIGHT, 1, left, OPP)
            hooks[0]()
            self.wait(PART, 0)
            self.send(PART, 0, right, PLEFT)
            self.send(PART, 0, left, PRIGHT)
            self.wait(PART, 1)
            self.send(PART, 1, left, PRIGHT)
            self.send(PART, 1, right, PLEFT)
            self.wait(LEFT, 1)
            self.wait(RIGHT, 0)
            hooks[1]()
            self.wait(PLEFT, 0)
            self.send(PLEFT, 0, right, POPP)
            self.wait(PRIGHT, 1)
            self.send(PRIGHT, 1, left, POPP)
            self.wait(OPP, 0)
            self.wait(OPP, 1)
            hooks[2]()
            self.wait(PLEFT, 1)
            self.wait(PRIGHT, 0)
            hooks[3]()
            self.wait(POPP, 0)
            self.wait(POPP, 1)
            hooks[4]()

        def drain(self):
            for c in self.sent:
                c.wait_send()

    ga = Gather(G, D1, a_send, a_recv)
    ga.start()

    tok = lax.broadcasted_iota(jnp.int32, (T, HD), 0) + cp * T
    first = jnp.zeros((T, HD), jnp.int32)
    run_start = jnp.int32(0)
    for j in range(seq.shape[0]):
        first = jnp.where(tok >= run_start, run_start, first)
        run_start = run_start + seq[j]
    START[...] = first
    angle = (tok - first).astype(F32) * freq[...]
    COS[...] = jnp.cos(angle)
    sgn = jnp.where(lax.broadcasted_iota(jnp.int32, (T, HD), 1) < HD // 2, -1.0, 1.0)
    SIN[...] = jnp.sin(angle) * sgn

    def slab(slot):
        return pl.ds(pl.multiple_of(tps[slot] * D1, 128), D1)

    def squares(slots, init=False):
        total = None if init else SS[...]
        for s in slots:
            v = G[:, slab(s)].astype(F32)
            v = v * v
            for c in range(D1 // HD):
                piece = v[:, c * HD:(c + 1) * HD]
                total = piece if total is None else total + piece
        SS[...] = total

    ga.run([
        lambda: squares((0,), True),
        lambda: squares((LEFT, RIGHT, PART)),
        lambda: squares((OPP,)),
        lambda: squares((PLEFT, PRIGHT)),
        lambda: squares((POPP,)),
    ])
    loads[0].wait()
    loads[1].wait()
    inv = lax.rsqrt(jnp.sum(SS[...], axis=1, keepdims=True) / (8.0 * D1) + EPS)
    pair = 2 * D1
    kv = None
    for i in range(4):
        sl = slice(i * pair, (i + 1) * pair)
        n = (G[:, sl].astype(F32) * inv * gain[:, sl]).astype(BF)
        N[:, sl] = n
        part = jnp.dot(n, W[sl, H1:], preferred_element_type=F32)
        kv = part if kv is None else kv + part

    def rope(u):
        return u * COS[...] + pltpu.roll(u, HD // 2, 1) * SIN[...]

    mine = cp
    knew = rope(kv[:, :HD] + bk[...].astype(F32)).astype(BF)
    vnew = (kv[:, HD:] + bv[...].astype(F32)).astype(BF)
    Kb[mine] = knew
    Vb[mine] = vnew
    kout[...] = knew
    vout[...] = vnew

    sent = []

    def piece(part, p, s, kk):
        blk = p * 16 + s * 2 + kk
        return (Kb if part == 0 else Vb).at[blk], kv_recv.at[part * 32 + blk]

    def send(cond, part, p, s, dev):
        r, rs = piece(part, p, s, k)
        c = pltpu.make_async_remote_copy(
            src_ref=r, dst_ref=r, send_sem=kv_send.at[len(sent)], recv_sem=rs,
            device_id=dev, device_id_type=MESH,
        )
        if cond is None:
            c.start()
        else:
            pl.when(cond)(c.start)
        sent.append((cond, c))

    def wait_for(cond, part, p, s, kk):
        r, rs = piece(part, p, s, kk)
        c = pltpu.make_async_remote_copy(
            src_ref=r, dst_ref=r, send_sem=kv_send.at[0], recv_sem=rs,
            device_id=sib, device_id_type=MESH,
        )
        if cond is None:
            c.wait_recv()
        else:
            pl.when(cond)(c.wait_recv)

    y0 = y == 0
    y1 = y == 1

    def up(kind, s, d):
        if kind == "KX":
            return y1
        low = s + d <= 7
        return jnp.logical_or(y0, low) if kind == "VO" else low

    def down(kind, s):
        if kind == "KX":
            return y1
        low = s <= 2
        return jnp.logical_or(y0, low) if kind == "VO" else low

    zero = jnp.int32(0)
    KINDS = (("KO", 0, y), ("VO", 1, y), ("KX", 0, zero))

    for part in (0, 1):
        kind = ("KO", "VO")[part]
        send(up(kind, z, 1), part, y, z, zplus)
        send(down(kind, z), part, y, z, zminus)
        send(y0, part, y, z, ypart)
        send(None, part, y, z, sib)

    loads[2].wait()
    q = jnp.dot(N[...], W[:, :H1], preferred_element_type=F32) + bq[...].astype(F32)
    for h in range(NH):
        Q[h] = rope(q[:, h * HD:(h + 1) * HD]).astype(BF)

    scale = HD ** (-0.5)

    def attend(p, s, diag):
        b0 = p * 16 + s * 2
        keys = Kb[pl.ds(b0, 2)].reshape(2 * T, HD)
        vals = Vb[pl.ds(b0, 2)].reshape(2 * T, HD)
        kpos = lax.broadcasted_iota(jnp.int32, (T, 2 * T), 1) + b0 * T
        allowed = kpos >= START[:, :1]
        if diag:
            qpos = lax.broadcasted_iota(jnp.int32, (T, 2 * T), 0) + cp * T
            allowed = jnp.logical_and(allowed, kpos <= qpos)
        for h in range(NH):
            sc = lax.dot_general(
                Q[h], keys, (((1,), (1,)), ((), ())), preferred_element_type=F32
            ) * scale
            sc = jnp.where(allowed, sc, NEG)
            top = jnp.max(sc, axis=1, keepdims=True)
            if not diag:
                top = jnp.maximum(top, M[h][:, :1])
            w = jnp.exp(sc - top)
            tot = w[:, :HD]
            for c in range(1, 2 * T // HD):
                tot = tot + w[:, c * HD:(c + 1) * HD]
            add = jnp.dot(w.astype(BF), vals, preferred_element_type=F32)
            if diag:
                L[h] = tot
                ACC[h] = add
            else:
                f = jnp.exp(M[h] - top)
                L[h] = L[h] * f + tot
                ACC[h] = ACC[h] * f + add
            M[h] = jnp.broadcast_to(top, (T, HD))

    def ring(d):
        s = lax.rem(z + 8 - d, 8)
        for kind, part, p in KINDS:
            got = up(kind, s, d)
            wait_for(got, part, p, s, k)
            if d < 4:
                send(up(kind, s, d + 1), part, p, s, zplus)
            if kind == "VO":
                send(y0, part, p, s, ypart)
            send(y1 if kind == "KX" else z - d >= 0, part, p, s, sib)
        if d < 4:
            s = lax.rem(z + d, 8)
            for kind, part, p in KINDS:
                got = down(kind, s)
                wait_for(got, part, p, s, k)
                if d < 3:
                    send(got, part, p, s, zminus)
                if kind == "VO":
                    send(y0, part, p, s, ypart)
                send(y1 if kind == "KX" else z + d >= 8, part, p, s, sib)

    def cross(d):
        for s in ([lax.rem(z + 8 - d, 8)] + ([lax.rem(z + d, 8)] if 0 < d < 4 else [])):
            wait_for(y1, 1, zero, s, k)
            send(y1, 1, zero, s, sib)

    def slabs(e, e2):
        def step(j, carry):
            i = lax.rem(j, 2)
            other = lax.div(j, 2)
            dist = e * (1 - other) + e2 * other
            v = z + (2 * i - 1) * dist
            s = lax.rem(v + 8, 8)
            p = y * (1 - other)
            two = lambda n: 0 < n < 4
            own_ok = v - 8 * i >= 0
            if not two(e):
                own_ok = jnp.logical_and(own_ok, i == 0) if e == 4 else (i < 0)
            oth_ok = y1
            if not two(e2):
                oth_ok = jnp.logical_and(y1, i == 0) if e2 in (0, 4) else (i < 0)
            cond = jnp.logical_or(
                jnp.logical_and(other == 0, own_ok), jnp.logical_and(other == 1, oth_ok)
            )

            @pl.when(cond)
            def _():
                wait_for(None, 0, p, s, 1 - k)
                wait_for(None, 1, p, s, 1 - k)
                attend(p, s, False)

            return carry

        lax.fori_loop(0, 4, step, 0)

    wait_for(y1, 0, zero, z, k)
    send(y1, 0, zero, z, zplus)
    send(y1, 0, zero, z, zminus)
    send(y1, 0, zero, z, sib)
    wait_for(None, 0, y, z, 1 - k)
    wait_for(None, 1, y, z, 1 - k)
    attend(y, z, True)
    for r in range(1, 7):
        if r <= 4:
            ring(r)
        if r <= 5:
            cross(r - 1)
        slabs(r - 1, r - 2)

    gc = Gather(AT, H1, c_send, c_recv)
    for h in range(NH):
        o = ACC[h] / jnp.sum(L[h], axis=1, keepdims=True)
        AT[:, pl.ds(pl.multiple_of(tp * H1 + h * HD, 128), HD)] = o.astype(BF)
    gc.start()
    loads[3].wait()
    OACC[...] = G[:, own_cols].astype(F32)

    def project(xi):
        rows = pl.ds(pl.multiple_of(xi * 2 * H1, 128), 2 * H1)
        OACC[...] += jnp.dot(AT[:, rows], Wo[rows, :], preferred_element_type=F32)

    gc.run([
        lambda: None,
        lambda: project(x),
        lambda: None,
        lambda: (project(xl), project(xr)),
        lambda: project(xo),
    ])
    mixed[...] = OACC[...].astype(BF)
    ga.drain()
    gc.drain()
    for cond, c in sent:
        if cond is None:
            c.wait_send()
        else:
            pl.when(cond)(c.wait_send)


def local(
    hidden_in, norm_gain, seq_lengths, w_query, b_query, w_key, b_key, w_value, b_value, w_out
):
    T, D1 = hidden_in.shape
    D = w_query.shape[0]
    H1 = w_query.shape[1]
    NH = H1 // HD
    f = ROPE_BASE ** (-jnp.arange(HD // 2, dtype=F32) / (HD // 2))
    freq = jnp.concatenate([f, f]).reshape(1, HD)
    vm = pl.BlockSpec(memory_space=pltpu.VMEM)
    hb = pl.BlockSpec(memory_space=pl.ANY)
    sm = pl.BlockSpec(memory_space=pltpu.SMEM)
    V = pltpu.VMEM
    return pl.pallas_call(
        kernel,
        out_shape=(
            jax.ShapeDtypeStruct((T, D1), BF),
            jax.ShapeDtypeStruct((T, HD), BF),
            jax.ShapeDtypeStruct((T, HD), BF),
        ),
        in_specs=[hb, vm, sm, hb, vm, hb, vm, hb, vm, hb, vm],
        out_specs=(vm, vm, vm),
        scratch_shapes=[
            V((T, D), BF), V((T, D), BF), V((D, H1 + 2 * HD), BF), V(w_out.shape, BF),
            V((32, T, HD), BF), V((32, T, HD), BF), V((T, 8 * H1), BF), V((NH, T, HD), BF),
            V((NH, T, HD), F32), V((NH, T, HD), F32), V((NH, T, HD), F32),
            V((T, HD), F32), V((T, HD), F32), V((T, HD), jnp.int32), V((T, HD), F32),
            V((T, D1), F32),
            pltpu.SemaphoreType.DMA((5,)),
            pltpu.SemaphoreType.DMA((14,)), pltpu.SemaphoreType.DMA((16,)),
            pltpu.SemaphoreType.DMA((14,)), pltpu.SemaphoreType.DMA((16,)),
            pltpu.SemaphoreType.DMA((SENDS,)), pltpu.SemaphoreType.DMA((64,)),
        ],
        compiler_params=pltpu.CompilerParams(
            collective_id=0, has_side_effects=True, vmem_limit_bytes=60 * 1024 * 1024
        ),
        name="layer",
    )(
        hidden_in, norm_gain.reshape(1, D), seq_lengths, w_query, b_query.reshape(1, H1),
        w_key, b_key.reshape(1, HD), w_value, b_value.reshape(1, HD), w_out, freq,
    )


def solution(mesh):
    placed = (
        P("cp", "tp"), P(), P(), P(None, "tp"), P("tp"), P(None, "tp"), P("tp"),
        P(None, "tp"), P("tp"), P(None, "tp"),
    )
    return jax.shard_map(
        local, mesh=mesh, in_specs=placed,
        out_specs=(P("cp", "tp"), P("cp", "tp"), P("cp", "tp")), check_vma=False,
    )
```

```python
import jax
import jax.numpy as jnp
import numpy as np
from jax import lax
from jax.experimental import pallas as pl
from jax.experimental.pallas import tpu as pltpu
from jax.sharding import PartitionSpec as P

HD = 128
EPS = 1e-06
ROPE_BASE = 1000000.0
FAR = -float(2**100)
LOG2E = 1.4426950408889634
MESH = pl.DeviceIdType.MESH
BF = jnp.bfloat16
F32 = jnp.float32
LEFT, RIGHT, OPP, PART, PLEFT, PRIGHT, POPP = 1, 2, 3, 4, 5, 6, 7
SENDS = 80


def kernel(
    hid, gain, seq, wq, bq, wk, bk, wv, bv, wo, freq,
    mixed, kout, vout,
    G, N, W, Wo, Kb, Vb, AT, Q, M, L, ACC, COS, SIN, QDOC, DOC, SS, OACC,
    lsem, a_send, a_recv, c_send, c_recv, kv_send, kv_recv,
):
    T = hid.shape[0]
    D1 = hid.shape[1]
    H1 = wo.shape[0] // 8
    NH = H1 // HD
    half = T // 2
    cp = lax.axis_index("cp")
    tp = lax.axis_index("tp")
    y = lax.div(cp, 16)
    z = lax.div(lax.rem(cp, 16), 2)
    k = lax.rem(cp, 2)
    x = lax.div(tp, 2)
    yh = lax.rem(tp, 2)
    xl = lax.rem(x + 3, 4)
    xr = lax.rem(x + 1, 4)
    xo = lax.rem(x + 2, 4)
    right = (cp, 2 * xr + yh)
    left = (cp, 2 * xl + yh)
    partner = (cp, 2 * x + 1 - yh)
    zplus = (y * 16 + lax.rem(z + 1, 8) * 2 + k, tp)
    zminus = (y * 16 + lax.rem(z + 7, 8) * 2 + k, tp)
    ypart = ((1 - y) * 16 + z * 2 + k, tp)
    sib = (y * 16 + z * 2 + 1 - k, tp)

    own_cols = pl.ds(pl.multiple_of(tp * D1, 128), D1)
    load_hid = pltpu.make_async_copy(hid, G.at[:, own_cols], lsem.at[0])
    load_hid.start()
    loads = [
        pltpu.make_async_copy(wk, W.at[:, pl.ds(H1, HD)], lsem.at[1]),
        pltpu.make_async_copy(wv, W.at[:, pl.ds(H1 + HD, HD)], lsem.at[2]),
        pltpu.make_async_copy(wq, W.at[:, pl.ds(0, H1)], lsem.at[3]),
        pltpu.make_async_copy(wo, Wo, lsem.at[4]),
    ]

    barrier = pltpu.get_barrier_semaphore()
    for dev in (right, left, partner, zplus, zminus, ypart, sib):
        pl.semaphore_signal(barrier, inc=1, device_id=dev, device_id_type=MESH)
    for c in loads:
        c.start()
    pl.semaphore_wait(barrier, 7)
    load_hid.wait()

    tps = {
        0: 2 * x + yh, LEFT: 2 * xl + yh, RIGHT: 2 * xr + yh, OPP: 2 * xo + yh,
        PART: 2 * x + 1 - yh, PLEFT: 2 * xl + 1 - yh, PRIGHT: 2 * xr + 1 - yh, POPP: 2 * xo + 1 - yh,
    }

    class Gather:
        def __init__(self, buf, width, ssem, rsem):
            self.buf, self.width, self.ssem, self.rsem = buf, width, ssem, rsem
            self.sent = []

        def ref(self, slot, h):
            cols = pl.ds(pl.multiple_of(tps[slot] * self.width, 128), self.width)
            return self.buf.at[pl.ds(h * half, half), cols]

        def send(self, slot, h, dev, dst_slot):
            r = self.ref(slot, h)
            c = pltpu.make_async_remote_copy(
                src_ref=r, dst_ref=r, send_sem=self.ssem.at[len(self.sent)],
                recv_sem=self.rsem.at[dst_slot * 2 + h], device_id=dev, device_id_type=MESH,
            )
            c.start()
            self.sent.append(c)

        def wait(self, slot, h):
            r = self.ref(slot, h)
            pltpu.make_async_remote_copy(
                src_ref=r, dst_ref=r, send_sem=self.ssem.at[0],
                recv_sem=self.rsem.at[slot * 2 + h], device_id=right, device_id_type=MESH,
            ).wait_recv()

        def start(self):
            self.send(0, 0, right, LEFT)
            self.send(0, 1, left, RIGHT)
            self.send(0, 0, partner, PART)
            self.send(0, 1, right, LEFT)
            self.send(0, 0, left, RIGHT)
            self.send(0, 1, partner, PART)

        def run(self, hooks):
            self.wait(LEFT, 0)
            self.send(LEFT, 0, right, OPP)
            self.wait(RIGHT, 1)
            self.send(RIGHT, 1, left, OPP)
            hooks[0]()
            self.wait(PART, 0)
            self.send(PART, 0, right, PLEFT)
            self.send(PART, 0, left, PRIGHT)
            self.wait(PART, 1)
            self.send(PART, 1, left, PRIGHT)
            self.send(PART, 1, right, PLEFT)
            self.wait(LEFT, 1)
            self.wait(RIGHT, 0)
            hooks[1]()
            self.wait(OPP, 0)
            self.send(OPP, 0, partner, POPP)
            self.wait(OPP, 1)
            self.send(OPP, 1, partner, POPP)
            hooks[2]()
            self.wait(PLEFT, 0)
            self.wait(PRIGHT, 1)
            self.wait(PLEFT, 1)
            self.wait(PRIGHT, 0)
            hooks[3]()
            self.wait(POPP, 0)
            self.wait(POPP, 1)
            hooks[4]()

        def drain(self):
            for c in self.sent:
                c.wait_send()

    ga = Gather(G, D1, a_send, a_recv)
    ga.start()

    lane = lax.broadcasted_iota(jnp.int32, (1, HD), 1)
    starts = jnp.full((1, HD), 1 << 30, jnp.int32)
    ends = jnp.zeros((1, HD), jnp.int32)
    tok = lax.broadcasted_iota(jnp.int32, (T, HD), 0) + cp * T
    first = jnp.zeros((T, HD), jnp.int32)
    edge = jnp.int32(0)
    for j in range(seq.shape[0]):
        first = jnp.where(tok >= edge, edge, first)
        starts = jnp.where(lane == j, edge, starts)
        edge = edge + seq[j]
        ends = jnp.where(lane == j, edge, ends)
    angle = (tok - first).astype(F32) * freq[...]
    COS[...] = jnp.cos(angle)
    sgn = jnp.where(lax.broadcasted_iota(jnp.int32, (T, HD), 1) < HD // 2, -1.0, 1.0)
    SIN[...] = jnp.sin(angle) * sgn
    inside = jnp.logical_and(tok >= starts, tok < ends)
    QDOC[...] = jnp.where(inside, FAR, 0.0).astype(BF)
    live = lane < seq.shape[0]

    def doc_block(i, carry):
        pos = lax.broadcasted_iota(jnp.int32, (T, HD), 0) + i * T
        out = jnp.logical_or(pos < starts, pos >= ends)
        DOC[i] = jnp.where(jnp.logical_and(out, live), 1.0, 0.0).astype(BF)
        return carry

    lax.fori_loop(0, DOC.shape[0], doc_block, 0)

    def slab(slot):
        return pl.ds(pl.multiple_of(tps[slot] * D1, 128), D1)

    def squares(slots, init=False):
        total = None if init else SS[...]
        for s in slots:
            v = G[:, slab(s)].astype(F32)
            v = v * v
            for c in range(D1 // HD):
                piece = v[:, c * HD:(c + 1) * HD]
                total = piece if total is None else total + piece
        SS[...] = total

    ga.run([
        lambda: squares((0,), True),
        lambda: squares((LEFT, RIGHT, PART)),
        lambda: squares((OPP,)),
        lambda: squares((PLEFT, PRIGHT)),
        lambda: squares((POPP,)),
    ])
    loads[0].wait()
    loads[1].wait()
    inv = lax.rsqrt(jnp.sum(SS[...], axis=1, keepdims=True) / (8.0 * D1) + EPS)
    pair = 2 * D1
    kv = None
    for i in range(4):
        sl = slice(i * pair, (i + 1) * pair)
        n = (G[:, sl].astype(F32) * inv * gain[:, sl]).astype(BF)
        N[:, sl] = n
        part = jnp.dot(n, W[sl, H1:], preferred_element_type=F32)
        kv = part if kv is None else kv + part

    def rope(u):
        return u * COS[...] + pltpu.roll(u, HD // 2, 1) * SIN[...]

    mine = cp
    knew = rope(kv[:, :HD] + bk[...].astype(F32)).astype(BF)
    vnew = (kv[:, HD:] + bv[...].astype(F32)).astype(BF)
    Kb[mine] = knew
    Vb[mine] = vnew
    kout[...] = knew
    vout[...] = vnew

    sent = []

    def piece(part, p, s, kk):
        blk = p * 16 + s * 2 + kk
        return (Kb if part == 0 else Vb).at[blk], kv_recv.at[part * 32 + blk]

    def send(cond, part, p, s, dev):
        r, rs = piece(part, p, s, k)
        c = pltpu.make_async_remote_copy(
            src_ref=r, dst_ref=r, send_sem=kv_send.at[len(sent)], recv_sem=rs,
            device_id=dev, device_id_type=MESH,
        )
        if cond is None:
            c.start()
        else:
            pl.when(cond)(c.start)
        sent.append((cond, c))

    def wait_for(cond, part, p, s, kk):
        r, rs = piece(part, p, s, kk)
        c = pltpu.make_async_remote_copy(
            src_ref=r, dst_ref=r, send_sem=kv_send.at[0], recv_sem=rs,
            device_id=sib, device_id_type=MESH,
        )
        if cond is None:
            c.wait_recv()
        else:
            pl.when(cond)(c.wait_recv)

    y0 = y == 0
    y1 = y == 1

    def up(kind, s, d):
        if kind == "KX":
            return y1
        low = s + d <= 7
        return jnp.logical_or(y0, low) if kind == "VO" else low

    def down(kind, s, d):
        if kind == "KX":
            return jnp.logical_and(y1, s - d >= 0)
        low = s <= 2
        return jnp.logical_or(y0, low) if kind == "VO" else low

    def seen(s):
        return s >= z - 4

    zero = jnp.int32(0)
    KINDS = (("KO", 0, y), ("VO", 1, y), ("KX", 0, zero))

    for part in (0, 1):
        kind = ("KO", "VO")[part]
        send(up(kind, z, 1), part, y, z, zplus)
        send(down(kind, z, 1), part, y, z, zminus)
        send(y0, part, y, z, ypart)
        send(None, part, y, z, sib)

    loads[2].wait()
    q = jnp.dot(N[...], W[:, :H1], preferred_element_type=F32)
    for h in range(NH):
        Q[h] = rope(q[:, h * HD:(h + 1) * HD] + bq[h:h + 1, :].astype(F32)).astype(BF)

    scale = HD ** (-0.5) * LOG2E

    def attend(p, s, diag):
        b0 = p * 16 + s * 2
        keys = jnp.concatenate(
            [Kb[pl.ds(b0, 2)].reshape(2 * T, HD), DOC[pl.ds(b0, 2)].reshape(2 * T, HD)], axis=1
        )
        vals = Vb[pl.ds(b0, 2)].reshape(2 * T, HD)
        for h in range(NH):
            sc = lax.dot_general(
                jnp.concatenate([Q[h], QDOC[...]], axis=1), keys, (((1,), (1,)), ((), ())),
                preferred_element_type=F32,
            )
            if diag:
                kpos = lax.broadcasted_iota(jnp.int32, (T, 2 * T), 1)
                qpos = lax.broadcasted_iota(jnp.int32, (T, 2 * T), 0) + k * T
                sc = jnp.where(kpos <= qpos, sc, FAR)
            top = jnp.max(sc, axis=1, keepdims=True)
            if not diag:
                top = jnp.maximum(top, M[h][:, :1])
            w = jnp.exp2((sc - top) * scale)
            tot = w[:, :HD]
            for c in range(1, 2 * T // HD):
                tot = tot + w[:, c * HD:(c + 1) * HD]
            add = jnp.dot(w.astype(BF), vals, preferred_element_type=F32)
            if diag:
                L[h] = tot
                ACC[h] = add
            else:
                f = jnp.exp2((M[h] - top) * scale)
                L[h] = L[h] * f + tot
                ACC[h] = ACC[h] * f + add
            M[h] = jnp.broadcast_to(top, (T, HD))

    def plus(d):
        s = lax.rem(z + 8 - d, 8)
        for kind, part, p in KINDS:
            wait_for(up(kind, s, d), part, p, s, k)
            if d < 4:
                send(up(kind, s, d + 1), part, p, s, zplus)
            if kind == "VO":
                send(jnp.logical_and(y0, seen(s)), part, p, s, ypart)
            send(y1 if kind == "KX" else z - d >= 0, part, p, s, sib)

    def minus(d):
        s = lax.rem(z + d, 8)
        for kind, part, p in KINDS:
            got = down(kind, s, d)
            wait_for(got, part, p, s, k)
            if d < 3:
                send(down(kind, s, d + 1), part, p, s, zminus)
            if kind == "VO":
                send(jnp.logical_and(y0, seen(s)), part, p, s, ypart)
            send(got if kind == "KX" else z + d >= 8, part, p, s, sib)

    def cross(s):
        here = jnp.logical_and(y1, seen(s))
        wait_for(here, 1, zero, s, k)
        send(here, 1, zero, s, sib)

    def near(d):
        return lax.rem(z + 8 - d, 8), lax.rem(z + d, 8)

    def visit(cond, p, s):
        @pl.when(cond)
        def _():
            wait_for(None, 0, p, s, 1 - k)
            wait_for(None, 1, p, s, 1 - k)
            attend(p, s, False)

    wait_for(y1, 0, zero, z, k)
    send(y1, 0, zero, z, zplus)
    send(down("KX", z, 1), 0, zero, z, zminus)
    send(y1, 0, zero, z, sib)
    wait_for(None, 0, y, z, 1 - k)
    wait_for(None, 1, y, z, 1 - k)
    attend(y, z, True)
    for r in range(1, 7):
        lo, hi = near(r - 1)
        lo2, hi2 = near(max(r - 2, 0))
        if r <= 4:
            plus(r)
        if 2 <= r <= 5:
            visit(z - (r - 1) >= 0, y, lo)
        if r <= 3:
            minus(r)
        if 2 <= r <= 4:
            visit(z + (r - 1) >= 8, y, hi)
        if r <= 5:
            cross(lo)
        if 2 <= r:
            visit(jnp.logical_and(y1, seen(lo2)), zero, lo2)
        if 2 <= r <= 4:
            cross(hi)
        if 3 <= r <= 5:
            visit(jnp.logical_and(y1, seen(hi2)), zero, hi2)

    gc = Gather(AT, H1, c_send, c_recv)
    for h in range(NH):
        o = ACC[h] / jnp.sum(L[h], axis=1, keepdims=True)
        AT[:, pl.ds(pl.multiple_of(tp * H1 + h * HD, 128), HD)] = o.astype(BF)
    gc.start()
    loads[3].wait()
    OACC[...] = G[:, own_cols].astype(F32)

    def project(xi):
        rows = pl.ds(pl.multiple_of(xi * 2 * H1, 128), 2 * H1)
        OACC[...] += jnp.dot(AT[:, rows], Wo[rows, :], preferred_element_type=F32)

    gc.run([
        lambda: None,
        lambda: project(x),
        lambda: None,
        lambda: (project(xl), project(xr)),
        lambda: project(xo),
    ])
    mixed[...] = OACC[...].astype(BF)
    ga.drain()
    gc.drain()
    for cond, c in sent:
        if cond is None:
            c.wait_send()
        else:
            pl.when(cond)(c.wait_send)


def finish(a, b, c, oa, ob, oc, va, vb, vc, sems):
    ins = [pltpu.make_async_copy(r, v, sems.at[i]) for i, (r, v) in enumerate(((b, vb), (c, vc), (a, va)))]
    outs = [pltpu.make_async_copy(v, o, sems.at[3 + i]) for i, (v, o) in enumerate(((vb, ob), (vc, oc), (va, oa)))]
    for c_in in ins:
        c_in.start()
    for c_in, c_out in zip(ins, outs):
        c_in.wait()
        c_out.start()
    for c_out in outs:
        c_out.wait()


def local(
    hidden_in, norm_gain, seq_lengths, w_query, b_query, w_key, b_key, w_value, b_value, w_out
):
    T, D1 = hidden_in.shape
    D = w_query.shape[0]
    H1 = w_query.shape[1]
    NH = H1 // HD
    f = (ROPE_BASE ** (-np.arange(HD // 2) / (HD // 2))).astype(np.float32)
    freq = jnp.asarray(np.concatenate([f, f]).reshape(1, HD))
    vm = pl.BlockSpec(memory_space=pltpu.VMEM)
    hb = pl.BlockSpec(memory_space=pl.ANY)
    sm = pl.BlockSpec(memory_space=pltpu.SMEM)
    V = pltpu.VMEM
    made = pl.pallas_call(
        kernel,
        out_shape=(
            jax.ShapeDtypeStruct((T, D1), BF),
            jax.ShapeDtypeStruct((T, HD), BF),
            jax.ShapeDtypeStruct((T, HD), BF),
        ),
        in_specs=[hb, vm, sm, hb, vm, hb, vm, hb, vm, hb, vm],
        out_specs=(vm, vm, vm),
        scratch_shapes=[
            V((T, D), BF), V((T, D), BF), V((D, H1 + 2 * HD), BF), V(w_out.shape, BF),
            V((32, T, HD), BF), V((32, T, HD), BF), V((T, 8 * H1), BF), V((NH, T, HD), BF),
            V((NH, T, HD), F32), V((NH, T, HD), F32), V((NH, T, HD), F32),
            V((T, HD), F32), V((T, HD), F32), V((T, HD), BF), V((32, T, HD), BF), V((T, HD), F32),
            V((T, D1), F32),
            pltpu.SemaphoreType.DMA((5,)),
            pltpu.SemaphoreType.DMA((14,)), pltpu.SemaphoreType.DMA((16,)),
            pltpu.SemaphoreType.DMA((14,)), pltpu.SemaphoreType.DMA((16,)),
            pltpu.SemaphoreType.DMA((SENDS,)), pltpu.SemaphoreType.DMA((64,)),
        ],
        compiler_params=pltpu.CompilerParams(
            collective_id=0, has_side_effects=True, vmem_limit_bytes=60 * 1024 * 1024
        ),
        name="layer",
    )(
        hidden_in, norm_gain.reshape(1, D), seq_lengths, w_query, b_query.reshape(NH, HD),
        w_key, b_key.reshape(1, HD), w_value, b_value.reshape(1, HD), w_out, freq,
    )
    return pl.pallas_call(
        finish,
        out_shape=tuple(jax.ShapeDtypeStruct(m.shape, m.dtype) for m in made),
        in_specs=[hb, hb, hb],
        out_specs=(hb, hb, hb),
        scratch_shapes=[V(m.shape, m.dtype) for m in made] + [pltpu.SemaphoreType.DMA((6,))],
        name="finish",
    )(*made)


def solution(mesh):
    placed = (
        P("cp", "tp"), P(), P(), P(None, "tp"), P("tp"), P(None, "tp"), P("tp"),
        P(None, "tp"), P("tp"), P(None, "tp"),
    )
    return jax.shard_map(
        local, mesh=mesh, in_specs=placed,
        out_specs=(P("cp", "tp"), P("cp", "tp"), P("cp", "tp")), check_vma=False,
    )
```

```python
import jax
import jax.numpy as jnp
import numpy as np
from jax import lax
from jax.experimental import pallas as pl
from jax.experimental.pallas import tpu as pltpu
from jax.sharding import PartitionSpec as P

HD = 128
EPS = 1e-06
ROPE_BASE = 1000000.0
FAR = -float(2**100)
LOG2E = 1.4426950408889634
MESH = pl.DeviceIdType.MESH
BF = jnp.bfloat16
F32 = jnp.float32
LEFT, RIGHT, OPP, PART, PLEFT, PRIGHT, POPP = 1, 2, 3, 4, 5, 6, 7
SENDS = 72


def kernel(
    hid, gain_h, seq_h, wq, bq_h, wk, bk_h, wv, bv_h, wo, freq_h,
    mixed, kout, vout,
    gain, bq, bk, bv, freq, seq, G, N, W, Wo, Kb, Vb, AT, Q, M, L, ACC, COS, SIN, QDOC, DOC, SS, OACC,
    lsem, a_send, a_recv, c_send, c_recv, kv_send, kv_recv,
):
    T = hid.shape[0]
    D1 = hid.shape[1]
    H1 = wo.shape[0] // 8
    NH = H1 // HD
    cp = lax.axis_index("cp")
    tp = lax.axis_index("tp")
    y = lax.div(cp, 16)
    z = lax.div(lax.rem(cp, 16), 2)
    k = lax.rem(cp, 2)
    x = lax.div(tp, 2)
    yh = lax.rem(tp, 2)
    xl = lax.rem(x + 3, 4)
    xr = lax.rem(x + 1, 4)
    xo = lax.rem(x + 2, 4)
    right = (cp, 2 * xr + yh)
    left = (cp, 2 * xl + yh)
    partner = (cp, 2 * x + 1 - yh)
    zplus = (y * 16 + lax.rem(z + 1, 8) * 2 + k, tp)
    zminus = (y * 16 + lax.rem(z + 7, 8) * 2 + k, tp)
    ypart = ((1 - y) * 16 + z * 2 + k, tp)
    sib = (y * 16 + z * 2 + 1 - k, tp)

    own_cols = pl.ds(pl.multiple_of(tp * D1, 128), D1)
    load_hid = pltpu.make_async_copy(hid, G.at[:, own_cols], lsem.at[0])
    load_hid.start()
    loads = [
        pltpu.make_async_copy(wk, W.at[:, pl.ds(H1, HD)], lsem.at[1]),
        pltpu.make_async_copy(wv, W.at[:, pl.ds(H1 + HD, HD)], lsem.at[2]),
        pltpu.make_async_copy(wq, W.at[:, pl.ds(0, H1)], lsem.at[3]),
        pltpu.make_async_copy(wo, Wo, lsem.at[4]),
    ]
    small = [
        pltpu.make_async_copy(a, b, lsem.at[5 + i])
        for i, (a, b) in enumerate(
            ((seq_h, seq), (freq_h, freq), (gain_h, gain), (bq_h, bq), (bk_h, bk), (bv_h, bv))
        )
    ]

    barrier = pltpu.get_barrier_semaphore()
    for dev in (right, left, partner, zplus, zminus, ypart, sib):
        pl.semaphore_signal(barrier, inc=1, device_id=dev, device_id_type=MESH)
    for c in small + loads:
        c.start()
    pl.semaphore_wait(barrier, 7)
    load_hid.wait()

    tps = {
        0: 2 * x + yh, LEFT: 2 * xl + yh, RIGHT: 2 * xr + yh, OPP: 2 * xo + yh,
        PART: 2 * x + 1 - yh, PLEFT: 2 * xl + 1 - yh, PRIGHT: 2 * xr + 1 - yh, POPP: 2 * xo + 1 - yh,
    }

    class Gather:
        def __init__(self, buf, width, ssem, rsem):
            self.buf, self.width, self.ssem, self.rsem = buf, width, ssem, rsem
            self.sent = []

        def ref(self, slot, c):
            cols = pl.ds(pl.multiple_of(tps[slot] * self.width, 128), self.width)
            return self.buf.at[pl.ds(c * (T // 4), T // 4), cols]

        def send(self, slot, c, dev, dst_slot):
            r = self.ref(slot, c)
            cpy = pltpu.make_async_remote_copy(
                src_ref=r, dst_ref=r, send_sem=self.ssem.at[len(self.sent)],
                recv_sem=self.rsem.at[dst_slot * 4 + c], device_id=dev, device_id_type=MESH,
            )
            cpy.start()
            self.sent.append(cpy)

        def wait(self, slot, *chunks):
            for c in chunks:
                r = self.ref(slot, c)
                pltpu.make_async_remote_copy(
                    src_ref=r, dst_ref=r, send_sem=self.ssem.at[0],
                    recv_sem=self.rsem.at[slot * 4 + c], device_id=right, device_id_type=MESH,
                ).wait_recv()

        def start(self):
            for c in (0, 1, 2):
                self.send(0, c, right, LEFT)
                self.send(0, (c + 2) % 4, left, RIGHT)
                self.send(0, c, partner, PART)
            self.send(0, 3, partner, PART)

        def pass_on(self, first):
            up, dn = (0, 2) if first else (1, 3)
            self.wait(LEFT, up)
            self.send(LEFT, up, right, OPP)
            self.wait(RIGHT, dn)
            self.send(RIGHT, dn, left, OPP)

        def rest(self):
            self.send(0, 3, right, LEFT)
            self.send(0, 1, left, RIGHT)

        def part(self, c):
            self.wait(PART, c)
            self.send(PART, c, right, PLEFT)
            self.send(PART, c, left, PRIGHT)

        def across(self, first):
            for c in ((0, 2) if first else (1, 3)):
                self.wait(OPP, c)
                self.send(OPP, c, partner, POPP)

        def drain(self):
            for c in self.sent:
                c.wait_send()

    ga = Gather(G, D1, a_send, a_recv)
    ga.start()

    for c in small:
        c.wait()

    lane = lax.broadcasted_iota(jnp.int32, (1, HD), 1)
    starts = jnp.full((1, HD), 1 << 30, jnp.int32)
    ends = jnp.zeros((1, HD), jnp.int32)
    tok = lax.broadcasted_iota(jnp.int32, (T, HD), 0) + cp * T
    first = jnp.zeros((T, HD), jnp.int32)
    edge = jnp.int32(0)
    for j in range(seq.shape[0]):
        first = jnp.where(tok >= edge, edge, first)
        starts = jnp.where(lane == j, edge, starts)
        edge = edge + seq[j]
        ends = jnp.where(lane == j, edge, ends)
    angle = (tok - first).astype(F32) * freq[...]
    COS[...] = jnp.cos(angle)
    sgn = jnp.where(lax.broadcasted_iota(jnp.int32, (T, HD), 1) < HD // 2, -1.0, 1.0)
    SIN[...] = jnp.sin(angle) * sgn
    inside = jnp.logical_and(tok >= starts, tok < ends)
    QDOC[...] = jnp.where(inside, FAR, 0.0).astype(BF)
    live = lane < seq.shape[0]

    def doc_block(i, carry):
        pos = lax.broadcasted_iota(jnp.int32, (T, HD), 0) + i * T
        out = jnp.logical_or(pos < starts, pos >= ends)
        DOC[i] = jnp.where(jnp.logical_and(out, live), 1.0, 0.0).astype(BF)
        return carry

    lax.fori_loop(0, DOC.shape[0], doc_block, 0)

    def slab(slot):
        return pl.ds(pl.multiple_of(tps[slot] * D1, 128), D1)

    def squares(slots, init=False):
        total = None if init else SS[...]
        for s in slots:
            v = G[:, slab(s)].astype(F32)
            v = v * v
            for c in range(D1 // HD):
                piece = v[:, c * HD:(c + 1) * HD]
                total = piece if total is None else total + piece
        SS[...] = total

    def rope(u):
        return u * COS[...] + pltpu.roll(u, HD // 2, 1) * SIN[...]

    def keys_values():
        inv = lax.rsqrt(jnp.sum(SS[...], axis=1, keepdims=True) / (8.0 * D1) + EPS)
        pair = 2 * D1
        kv = None
        for i in range(4):
            sl = slice(i * pair, (i + 1) * pair)
            n = (G[:, sl].astype(F32) * inv * gain[:, sl]).astype(BF)
            N[:, sl] = n
            part = jnp.dot(n, W[sl, H1:], preferred_element_type=F32)
            kv = part if kv is None else kv + part
        knew = rope(kv[:, :HD] + bk[...].astype(F32)).astype(BF)
        vnew = (kv[:, HD:] + bv[...].astype(F32)).astype(BF)
        Kb[cp] = knew
        Vb[cp] = vnew
        kout[...] = knew
        vout[...] = vnew

    def queries():
        q = jnp.dot(N[...], W[:, :H1], preferred_element_type=F32)
        for h in range(NH):
            Q[h] = rope(q[:, h * HD:(h + 1) * HD] + bq[h:h + 1, :].astype(F32)).astype(BF)

    sent = []

    def piece(part, p, s, kk):
        blk = p * 16 + s * 2 + kk
        return (Kb if part == 0 else Vb).at[blk], kv_recv.at[part * 32 + blk]

    def send(cond, part, p, s, dev):
        r, rs = piece(part, p, s, k)
        c = pltpu.make_async_remote_copy(
            src_ref=r, dst_ref=r, send_sem=kv_send.at[len(sent)], recv_sem=rs,
            device_id=dev, device_id_type=MESH,
        )
        if cond is None:
            c.start()
        else:
            pl.when(cond)(c.start)
        sent.append((cond, c))

    def wait_for(cond, part, p, s, kk):
        r, rs = piece(part, p, s, kk)
        c = pltpu.make_async_remote_copy(
            src_ref=r, dst_ref=r, send_sem=kv_send.at[0], recv_sem=rs,
            device_id=sib, device_id_type=MESH,
        )
        if cond is None:
            c.wait_recv()
        else:
            pl.when(cond)(c.wait_recv)

    scale = HD ** (-0.5) * LOG2E

    def attend(p, s, diag):
        b0 = p * 16 + s * 2
        keys = jnp.concatenate(
            [Kb[pl.ds(b0, 2)].reshape(2 * T, HD), DOC[pl.ds(b0, 2)].reshape(2 * T, HD)], axis=1
        )
        vals = Vb[pl.ds(b0, 2)].reshape(2 * T, HD)
        qs = jnp.concatenate([jnp.concatenate([Q[h], QDOC[...]], axis=1) for h in range(NH)], axis=0)
        sc = lax.dot_general(qs, keys, (((1,), (1,)), ((), ())), preferred_element_type=F32)
        if diag:
            kpos = lax.broadcasted_iota(jnp.int32, (T, 2 * T), 1)
            qpos = lax.broadcasted_iota(jnp.int32, (T, 2 * T), 0) + k * T
            sc = jnp.concatenate([jnp.where(kpos <= qpos, sc[h * T:(h + 1) * T], FAR) for h in range(NH)], axis=0)
        top = jnp.max(sc, axis=1, keepdims=True)
        m_old = M[...].reshape(NH * T, HD)
        if not diag:
            top = jnp.maximum(top, m_old[:, :1])
        w = jnp.exp2((sc - top) * scale)
        tot = w[:, :HD]
        for c in range(1, 2 * T // HD):
            tot = tot + w[:, c * HD:(c + 1) * HD]
        add = jnp.dot(w.astype(BF), vals, preferred_element_type=F32)
        if not diag:
            f = jnp.exp2((m_old - top) * scale)
            tot = L[...].reshape(NH * T, HD) * f + tot
            add = ACC[...].reshape(NH * T, HD) * f + add
        L[...] = tot.reshape(NH, T, HD)
        ACC[...] = add.reshape(NH, T, HD)
        M[...] = jnp.broadcast_to(top, (NH * T, HD)).reshape(NH, T, HD)

    y0 = y == 0
    y1 = y == 1
    zero = jnp.int32(0)
    KINDS = (("KO", 0, y), ("VO", 1, y), ("KX", 0, zero))

    def up(kind, s, d):
        low = s + d <= 7
        if kind == "KX":
            return y1 if d <= 4 else None
        if kind == "KO":
            return low if d <= 3 else None
        return jnp.logical_or(y0, low) if d <= 3 else (y0 if d == 4 else None)

    def down(kind, s, d):
        if kind == "KX":
            return jnp.logical_and(y1, s - d >= 0) if d <= 3 else None
        if kind == "KO":
            return s <= 3 if d <= 4 else None
        return jnp.logical_or(y0, s <= 3) if d <= 3 else (jnp.logical_and(y1, s <= 3) if d == 4 else None)

    def seen(s):
        return s >= z - 4

    def own():
        for part in (0, 1):
            kind = ("KO", "VO")[part]
            send(up(kind, z, 1), part, y, z, zplus)
            send(down(kind, z, 1), part, y, z, zminus)
            send(y0, part, y, z, ypart)
            send(None, part, y, z, sib)

    def first_key():
        wait_for(y1, 0, zero, z, k)
        send(y1, 0, zero, z, zplus)
        send(down("KX", z, 1), 0, zero, z, zminus)
        send(y1, 0, zero, z, sib)

    def hop(d, step, go, dev, mine):
        s = lax.rem(z + 8 + step * d, 8)
        for kind, part, p in KINDS:
            got = go(kind, s, d)
            if got is None:
                continue
            wait_for(got, part, p, s, k)
            on = go(kind, s, d + 1)
            if on is not None:
                send(on, part, p, s, dev)
            if kind == "VO" and (d <= 3 or step < 0):
                send(jnp.logical_and(y0, seen(s)), part, p, s, ypart)
            send(got if kind == "KX" else jnp.logical_and(got, mine), part, p, s, sib)

    def plus(d):
        hop(d, -1, up, zplus, z - d >= 0)

    def minus(d):
        hop(d, 1, down, zminus, z + d >= 8)

    def cross(s):
        here = jnp.logical_and(y1, seen(s))
        wait_for(here, 1, zero, s, k)
        send(here, 1, zero, s, sib)

    def lo(d):
        return lax.rem(z + 8 - d, 8)

    def hi(d):
        return lax.rem(z + d, 8)

    def visit(cond, p, s):
        @pl.when(cond)
        def _():
            wait_for(None, 0, p, s, 1 - k)
            wait_for(None, 1, p, s, 1 - k)
            attend(p, s, False)

    ga.pass_on(True)
    ga.rest()
    squares((0,), True)
    ga.pass_on(False)
    ga.part(0)
    ga.part(1)
    ga.across(True)
    ga.part(2)
    ga.part(3)
    ga.wait(LEFT, 2, 3)
    ga.wait(RIGHT, 0, 1)
    squares((LEFT, RIGHT))
    ga.across(False)
    squares((PART, OPP))
    ga.wait(PLEFT, 0, 1, 2, 3)
    ga.wait(PRIGHT, 0, 1, 2, 3)
    squares((PLEFT, PRIGHT))
    ga.wait(POPP, 0, 1, 2, 3)
    squares((POPP,))
    loads[0].wait()
    loads[1].wait()
    keys_values()
    own()
    loads[2].wait()
    queries()
    first_key()
    wait_for(None, 0, y, z, 1 - k)
    wait_for(None, 1, y, z, 1 - k)
    attend(y, z, True)
    plus(1)
    minus(1)
    cross(z)
    plus(2)
    visit(z - 1 >= 0, y, lo(1))
    minus(2)
    visit(z + 1 >= 8, y, hi(1))
    cross(lo(1))
    visit(y1, zero, z)
    cross(hi(1))
    plus(3)
    visit(z - 2 >= 0, y, lo(2))
    minus(3)
    visit(z + 2 >= 8, y, hi(2))
    cross(lo(2))
    visit(jnp.logical_and(y1, seen(lo(1))), zero, lo(1))
    cross(hi(2))
    visit(jnp.logical_and(y1, seen(hi(1))), zero, hi(1))
    plus(4)
    visit(z - 3 >= 0, y, lo(3))
    minus(4)
    visit(z + 3 >= 8, y, hi(3))
    cross(lo(3))
    visit(jnp.logical_and(y1, seen(lo(2))), zero, lo(2))
    cross(hi(3))
    visit(jnp.logical_and(y1, seen(hi(2))), zero, hi(2))
    cross(lo(4))
    visit(z + 4 >= 8, y, hi(4))
    visit(jnp.logical_and(y1, seen(lo(3))), zero, lo(3))
    visit(jnp.logical_and(y1, seen(hi(3))), zero, hi(3))
    visit(jnp.logical_and(y1, seen(lo(4))), zero, lo(4))

    gc = Gather(AT, H1, c_send, c_recv)
    for h in range(NH):
        o = ACC[h] / jnp.sum(L[h], axis=1, keepdims=True)
        AT[:, pl.ds(pl.multiple_of(tp * H1 + h * HD, 128), HD)] = o.astype(BF)
    gc.start()
    loads[3].wait()
    OACC[...] = G[:, own_cols].astype(F32)

    def project(xi):
        rows = pl.ds(pl.multiple_of(xi * 2 * H1, 128), 2 * H1)
        OACC[...] += jnp.dot(AT[:, rows], Wo[rows, :], preferred_element_type=F32)

    gc.pass_on(True)
    gc.rest()
    gc.pass_on(False)
    gc.part(0)
    gc.part(1)
    gc.across(True)
    gc.part(2)
    gc.part(3)
    project(x)
    gc.across(False)
    gc.wait(LEFT, 2, 3)
    gc.wait(RIGHT, 0, 1)
    gc.wait(PLEFT, 0, 1, 2, 3)
    gc.wait(PRIGHT, 0, 1, 2, 3)
    project(xl)
    project(xr)
    gc.wait(POPP, 0, 1, 2, 3)
    project(xo)
    mixed[...] = OACC[...].astype(BF)
    ga.drain()
    gc.drain()
    for cond, c in sent:
        if cond is None:
            c.wait_send()
        else:
            pl.when(cond)(c.wait_send)


def finish(a, b, c, oa, ob, oc, va, vb, vc, sems):
    ins = [pltpu.make_async_copy(r, v, sems.at[i]) for i, (r, v) in enumerate(((b, vb), (c, vc), (a, va)))]
    outs = [pltpu.make_async_copy(v, o, sems.at[3 + i]) for i, (v, o) in enumerate(((vb, ob), (vc, oc), (va, oa)))]
    for c_in in ins:
        c_in.start()
    for c_in, c_out in zip(ins, outs):
        c_in.wait()
        c_out.start()
    for c_out in outs:
        c_out.wait()


def local(
    hidden_in, norm_gain, seq_lengths, w_query, b_query, w_key, b_key, w_value, b_value, w_out
):
    T, D1 = hidden_in.shape
    D = w_query.shape[0]
    H1 = w_query.shape[1]
    NH = H1 // HD
    f = (ROPE_BASE ** (-np.arange(HD // 2) / (HD // 2))).astype(np.float32)
    freq = jnp.asarray(np.concatenate([f, f]).reshape(1, HD))
    vm = pl.BlockSpec(memory_space=pltpu.VMEM)
    hb = pl.BlockSpec(memory_space=pl.ANY)
    V = pltpu.VMEM
    made = pl.pallas_call(
        kernel,
        out_shape=(
            jax.ShapeDtypeStruct((T, D1), BF),
            jax.ShapeDtypeStruct((T, HD), BF),
            jax.ShapeDtypeStruct((T, HD), BF),
        ),
        in_specs=[hb] * 11,
        out_specs=(vm, vm, vm),
        scratch_shapes=[
            V((1, D), F32), V((NH, HD), BF), V((1, HD), BF), V((1, HD), BF), V((1, HD), F32),
            pltpu.SMEM(seq_lengths.shape, jnp.int32),
            V((T, D), BF), V((T, D), BF), V((D, H1 + 2 * HD), BF), V(w_out.shape, BF),
            V((32, T, HD), BF), V((32, T, HD), BF), V((T, 8 * H1), BF), V((NH, T, HD), BF),
            V((NH, T, HD), F32), V((NH, T, HD), F32), V((NH, T, HD), F32),
            V((T, HD), F32), V((T, HD), F32), V((T, HD), BF), V((32, T, HD), BF), V((T, HD), F32),
            V((T, D1), F32),
            pltpu.SemaphoreType.DMA((11,)),
            pltpu.SemaphoreType.DMA((28,)), pltpu.SemaphoreType.DMA((32,)),
            pltpu.SemaphoreType.DMA((28,)), pltpu.SemaphoreType.DMA((32,)),
            pltpu.SemaphoreType.DMA((SENDS,)), pltpu.SemaphoreType.DMA((64,)),
        ],
        compiler_params=pltpu.CompilerParams(
            collective_id=0, has_side_effects=True, vmem_limit_bytes=60 * 1024 * 1024
        ),
        name="layer",
    )(
        hidden_in, norm_gain.reshape(1, D), seq_lengths, w_query, b_query.reshape(NH, HD),
        w_key, b_key.reshape(1, HD), w_value, b_value.reshape(1, HD), w_out, freq,
    )
    return pl.pallas_call(
        finish,
        out_shape=tuple(jax.ShapeDtypeStruct(m.shape, m.dtype) for m in made),
        in_specs=[hb, hb, hb],
        out_specs=(hb, hb, hb),
        scratch_shapes=[V(m.shape, m.dtype) for m in made] + [pltpu.SemaphoreType.DMA((6,))],
        name="finish",
    )(*made)


def solution(mesh):
    placed = (
        P("cp", "tp"), P(), P(), P(None, "tp"), P("tp"), P(None, "tp"), P("tp"),
        P(None, "tp"), P("tp"), P(None, "tp"),
    )
    return jax.shard_map(
        local, mesh=mesh, in_specs=placed,
        out_specs=(P("cp", "tp"), P("cp", "tp"), P("cp", "tp")), check_vma=False,
    )
```

```python
import jax
import jax.numpy as jnp
import numpy as np
from jax import lax
from jax.experimental import pallas as pl
from jax.experimental.pallas import tpu as pltpu
from jax.sharding import PartitionSpec as P

HD = 128
EPS = 1e-06
ROPE_BASE = 1000000.0
FAR = -float(2**100)
LOG2E = 1.4426950408889634
MESH = pl.DeviceIdType.MESH
BF = jnp.bfloat16
F32 = jnp.float32
LEFT, RIGHT, OPP, PART, PLEFT, PRIGHT, POPP = 1, 2, 3, 4, 5, 6, 7
SENDS = 72


def kernel(
    hid, gain_h, seq_h, wq, bq_h, wk, bk_h, wv, bv_h, wo, freq_h,
    mixed, kout, vout,
    gain, bq, bk, bv, freq, seq, G, N, W, Wo, Kb, Vb, AT, Q, M, L, ACC, COS, SIN, QDOC, DOC, SS, OACC, MIX,
    lsem, a_send, a_recv, c_send, c_recv, kv_send, kv_recv,
):
    T = hid.shape[0]
    D1 = hid.shape[1]
    H1 = wo.shape[0] // 8
    NH = H1 // HD
    cp = lax.axis_index("cp")
    tp = lax.axis_index("tp")
    y = lax.div(cp, 16)
    z = lax.div(lax.rem(cp, 16), 2)
    k = lax.rem(cp, 2)
    x = lax.div(tp, 2)
    yh = lax.rem(tp, 2)
    xl = lax.rem(x + 3, 4)
    xr = lax.rem(x + 1, 4)
    xo = lax.rem(x + 2, 4)
    right = (cp, 2 * xr + yh)
    left = (cp, 2 * xl + yh)
    partner = (cp, 2 * x + 1 - yh)
    zplus = (y * 16 + lax.rem(z + 1, 8) * 2 + k, tp)
    zminus = (y * 16 + lax.rem(z + 7, 8) * 2 + k, tp)
    ypart = ((1 - y) * 16 + z * 2 + k, tp)
    sib = (y * 16 + z * 2 + 1 - k, tp)
    diag = ((1 - y) * 16 + lax.rem(z + 1 + 6 * y, 8) * 2 + k, tp)

    own_cols = pl.ds(pl.multiple_of(tp * D1, 128), D1)
    quarters = [pl.ds(i * (T // 4), T // 4) for i in range(4)]
    load_hid = [
        pltpu.make_async_copy(hid.at[q, :], G.at[q, own_cols], lsem.at[11 + i]) for i, q in enumerate(quarters)
    ]
    for c in load_hid:
        c.start()
    loads = [
        pltpu.make_async_copy(wk, W.at[:, pl.ds(H1, HD)], lsem.at[1]),
        pltpu.make_async_copy(wv, W.at[:, pl.ds(H1 + HD, HD)], lsem.at[2]),
        pltpu.make_async_copy(wq, W.at[:, pl.ds(0, H1)], lsem.at[3]),
        pltpu.make_async_copy(wo, Wo, lsem.at[4]),
    ]
    small = [
        pltpu.make_async_copy(a, b, lsem.at[5 + i])
        for i, (a, b) in enumerate(
            ((seq_h, seq), (freq_h, freq), (gain_h, gain), (bq_h, bq), (bk_h, bk), (bv_h, bv))
        )
    ]

    written = [
        pltpu.make_async_copy(Kb.at[cp], kout, lsem.at[15]),
        pltpu.make_async_copy(Vb.at[cp], vout, lsem.at[16]),
    ] + [
        pltpu.make_async_copy(MIX.at[q, :], mixed.at[q, :], lsem.at[17 + i]) for i, q in enumerate(quarters)
    ]

    barrier = pltpu.get_barrier_semaphore()
    for dev in (right, left, partner, zplus, zminus, ypart, sib, diag):
        pl.semaphore_signal(barrier, inc=1, device_id=dev, device_id_type=MESH)
    for c in small + loads:
        c.start()
    pl.semaphore_wait(barrier, 8)
    for c in load_hid:
        c.wait()

    tps = {
        0: 2 * x + yh, LEFT: 2 * xl + yh, RIGHT: 2 * xr + yh, OPP: 2 * xo + yh,
        PART: 2 * x + 1 - yh, PLEFT: 2 * xl + 1 - yh, PRIGHT: 2 * xr + 1 - yh, POPP: 2 * xo + 1 - yh,
    }

    class Gather:
        def __init__(self, buf, width, ssem, rsem):
            self.buf, self.width, self.ssem, self.rsem = buf, width, ssem, rsem
            self.sent = []

        def ref(self, slot, c):
            cols = pl.ds(pl.multiple_of(tps[slot] * self.width, 128), self.width)
            return self.buf.at[pl.ds(c * (T // 4), T // 4), cols]

        def send(self, slot, c, dev, dst_slot):
            r = self.ref(slot, c)
            cpy = pltpu.make_async_remote_copy(
                src_ref=r, dst_ref=r, send_sem=self.ssem.at[len(self.sent)],
                recv_sem=self.rsem.at[dst_slot * 4 + c], device_id=dev, device_id_type=MESH,
            )
            cpy.start()
            self.sent.append(cpy)

        def wait(self, slot, *chunks):
            for c in chunks:
                r = self.ref(slot, c)
                pltpu.make_async_remote_copy(
                    src_ref=r, dst_ref=r, send_sem=self.ssem.at[0],
                    recv_sem=self.rsem.at[slot * 4 + c], device_id=right, device_id_type=MESH,
                ).wait_recv()

        def start(self):
            for c in (0, 1, 2):
                self.send(0, c, right, LEFT)
                self.send(0, (c + 2) % 4, left, RIGHT)
                self.send(0, c, partner, PART)
            self.send(0, 3, partner, PART)

        def pass_on(self, first):
            up, dn = (0, 2) if first else (1, 3)
            self.wait(LEFT, up)
            self.send(LEFT, up, right, OPP)
            self.wait(RIGHT, dn)
            self.send(RIGHT, dn, left, OPP)

        def rest(self):
            self.send(0, 3, right, LEFT)
            self.send(0, 1, left, RIGHT)

        def part(self, c):
            self.wait(PART, c)
            self.send(PART, c, right, PLEFT)
            self.send(PART, c, left, PRIGHT)

        def across(self, first):
            for c in ((0, 2) if first else (1, 3)):
                self.wait(OPP, c)
                self.send(OPP, c, partner, POPP)

        def drain(self):
            for c in self.sent:
                c.wait_send()

    ga = Gather(G, D1, a_send, a_recv)
    ga.start()

    for c in small:
        c.wait()

    lane = lax.broadcasted_iota(jnp.int32, (1, HD), 1)
    starts = jnp.full((1, HD), 1 << 30, jnp.int32)
    ends = jnp.zeros((1, HD), jnp.int32)
    tok = lax.broadcasted_iota(jnp.int32, (T, HD), 0) + cp * T
    first = jnp.zeros((T, HD), jnp.int32)
    edge = jnp.int32(0)
    for j in range(seq.shape[0]):
        first = jnp.where(tok >= edge, edge, first)
        starts = jnp.where(lane == j, edge, starts)
        edge = edge + seq[j]
        ends = jnp.where(lane == j, edge, ends)
    angle = (tok - first).astype(F32) * freq[...]
    COS[...] = jnp.cos(angle)
    sgn = jnp.where(lax.broadcasted_iota(jnp.int32, (T, HD), 1) < HD // 2, -1.0, 1.0)
    SIN[...] = jnp.sin(angle) * sgn
    inside = jnp.logical_and(tok >= starts, tok < ends)
    QDOC[...] = jnp.where(inside, FAR, 0.0).astype(BF)
    live = lane < seq.shape[0]

    def doc_block(i, carry):
        pos = lax.broadcasted_iota(jnp.int32, (T, HD), 0) + i * T
        out = jnp.logical_or(pos < starts, pos >= ends)
        DOC[i] = jnp.where(jnp.logical_and(out, live), 1.0, 0.0).astype(BF)
        return carry

    lax.fori_loop(0, DOC.shape[0], doc_block, 0)

    def slab(slot):
        return pl.ds(pl.multiple_of(tps[slot] * D1, 128), D1)

    def squares(slots, init=False):
        total = None if init else SS[...]
        for s in slots:
            v = G[:, slab(s)].astype(F32)
            v = v * v
            for c in range(D1 // HD):
                piece = v[:, c * HD:(c + 1) * HD]
                total = piece if total is None else total + piece
        SS[...] = total

    def rope(u):
        return u * COS[...] + pltpu.roll(u, HD // 2, 1) * SIN[...]

    def keys_values():
        inv = lax.rsqrt(jnp.sum(SS[...], axis=1, keepdims=True) / (8.0 * D1) + EPS)
        pair = 2 * D1
        kv = None
        for i in range(4):
            sl = slice(i * pair, (i + 1) * pair)
            n = (G[:, sl].astype(F32) * inv * gain[:, sl]).astype(BF)
            N[:, sl] = n
            part = jnp.dot(n, W[sl, H1:], preferred_element_type=F32)
            kv = part if kv is None else kv + part
        knew = rope(kv[:, :HD] + bk[...].astype(F32)).astype(BF)
        vnew = (kv[:, HD:] + bv[...].astype(F32)).astype(BF)
        Kb[cp] = knew
        Vb[cp] = vnew
        for c in written[:2]:
            c.start()

    def queries():
        q = jnp.dot(N[...], W[:, :H1], preferred_element_type=F32)
        for h in range(NH):
            Q[h] = rope(q[:, h * HD:(h + 1) * HD] + bq[h:h + 1, :].astype(F32)).astype(BF)

    sent = []

    def piece(part, p, s, kk):
        blk = p * 16 + s * 2 + kk
        return (Kb if part == 0 else Vb).at[blk], kv_recv.at[part * 32 + blk]

    def send(cond, part, p, s, dev):
        r, rs = piece(part, p, s, k)
        c = pltpu.make_async_remote_copy(
            src_ref=r, dst_ref=r, send_sem=kv_send.at[len(sent)], recv_sem=rs,
            device_id=dev, device_id_type=MESH,
        )
        if cond is None:
            c.start()
        else:
            pl.when(cond)(c.start)
        sent.append((cond, c))

    def wait_for(cond, part, p, s, kk):
        r, rs = piece(part, p, s, kk)
        c = pltpu.make_async_remote_copy(
            src_ref=r, dst_ref=r, send_sem=kv_send.at[0], recv_sem=rs,
            device_id=sib, device_id_type=MESH,
        )
        if cond is None:
            c.wait_recv()
        else:
            pl.when(cond)(c.wait_recv)

    scale = HD ** (-0.5) * LOG2E

    def attend(p, s, diag):
        b0 = p * 16 + s * 2
        keys = jnp.concatenate(
            [Kb[pl.ds(b0, 2)].reshape(2 * T, HD), DOC[pl.ds(b0, 2)].reshape(2 * T, HD)], axis=1
        )
        vals = Vb[pl.ds(b0, 2)].reshape(2 * T, HD)
        qs = jnp.concatenate([jnp.concatenate([Q[h], QDOC[...]], axis=1) for h in range(NH)], axis=0)
        sc = lax.dot_general(qs, keys, (((1,), (1,)), ((), ())), preferred_element_type=F32)
        if diag:
            kpos = lax.broadcasted_iota(jnp.int32, (T, 2 * T), 1)
            qpos = lax.broadcasted_iota(jnp.int32, (T, 2 * T), 0) + k * T
            sc = jnp.concatenate([jnp.where(kpos <= qpos, sc[h * T:(h + 1) * T], FAR) for h in range(NH)], axis=0)
        top = jnp.max(sc, axis=1, keepdims=True)
        m_old = M[...].reshape(NH * T, HD)
        if not diag:
            top = jnp.maximum(top, m_old[:, :1])
        w = jnp.exp2((sc - top) * scale)
        tot = w[:, :HD]
        for c in range(1, 2 * T // HD):
            tot = tot + w[:, c * HD:(c + 1) * HD]
        add = jnp.dot(w.astype(BF), vals, preferred_element_type=F32)
        if not diag:
            f = jnp.exp2((m_old - top) * scale)
            tot = L[...].reshape(NH * T, HD) * f + tot
            add = ACC[...].reshape(NH * T, HD) * f + add
        L[...] = tot.reshape(NH, T, HD)
        ACC[...] = add.reshape(NH, T, HD)
        M[...] = jnp.broadcast_to(top, (NH * T, HD)).reshape(NH, T, HD)

    y0 = y == 0
    y1 = y == 1
    zero = jnp.int32(0)
    KINDS = (("KO", 0, y), ("VO", 1, y), ("KX", 0, zero))

    def up(kind, s, d):
        low = s + d <= 7
        if kind == "KX":
            return y1 if d <= 4 else None
        if kind == "KO":
            return low if d <= 3 else None
        return jnp.logical_or(y0, low) if d <= 3 else (jnp.logical_and(y0, low) if d == 4 else None)

    def down(kind, s, d):
        if kind == "KX":
            return jnp.logical_and(y1, s - d >= 0) if d <= 3 else None
        if kind == "KO":
            return s <= 3 if d <= 4 else None
        return jnp.logical_or(y0, s <= 3) if d <= 3 else (jnp.logical_and(y1, s <= 3) if d == 4 else None)

    def seen(s):
        return s >= z - 4

    def own():
        for part in (0, 1):
            kind = ("KO", "VO")[part]
            send(up(kind, z, 1), part, y, z, zplus)
            send(down(kind, z, 1), part, y, z, zminus)
            if part == 0:
                send(y0, part, y, z, diag)
            send(y0, part, y, z, ypart)
            send(None, part, y, z, sib)

    def first_key():
        wait_for(y1, 0, zero, z, k)
        send(down("KX", z, 1), 0, zero, z, zminus)
        send(y1, 0, zero, z, sib)

    def hop(d, step, go, dev, mine):
        s = lax.rem(z + 8 + step * d, 8)
        for kind, part, p in KINDS:
            got = go(kind, s, d)
            if got is None:
                continue
            wait_for(got, part, p, s, k)
            on = go(kind, s, d + 1)
            if on is not None:
                send(on, part, p, s, dev)
            if kind == "VO" and step < 0 and d == 3:
                send(y0, part, p, s, diag)
            if kind == "VO" and d <= 3:
                send(jnp.logical_and(y0, seen(s)), part, p, s, ypart)
            send(got if kind == "KX" else jnp.logical_and(got, mine), part, p, s, sib)

    def plus(d):
        hop(d, -1, up, zplus, z - d >= 0)

    def minus(d):
        hop(d, 1, down, zminus, z + d >= 8)

    def cross(s):
        here = jnp.logical_and(y1, seen(s))
        wait_for(here, 1, zero, s, k)
        send(here, 1, zero, s, sib)

    def lo(d):
        return lax.rem(z + 8 - d, 8)

    def hi(d):
        return lax.rem(z + d, 8)

    def visit(cond, p, s):
        @pl.when(cond)
        def _():
            wait_for(None, 0, p, s, 1 - k)
            wait_for(None, 1, p, s, 1 - k)
            attend(p, s, False)

    ga.pass_on(True)
    ga.rest()
    squares((0,), True)
    ga.pass_on(False)
    ga.part(0)
    ga.part(1)
    ga.across(True)
    ga.part(2)
    ga.part(3)
    ga.wait(LEFT, 2, 3)
    ga.wait(RIGHT, 0, 1)
    squares((LEFT, RIGHT))
    ga.across(False)
    squares((PART, OPP))
    ga.wait(PLEFT, 0, 1, 2, 3)
    ga.wait(PRIGHT, 0, 1, 2, 3)
    squares((PLEFT, PRIGHT))
    ga.wait(POPP, 0, 1, 2, 3)
    squares((POPP,))
    loads[0].wait()
    loads[1].wait()
    keys_values()
    own()
    loads[2].wait()
    queries()
    first_key()
    wait_for(None, 0, y, z, 1 - k)
    wait_for(None, 1, y, z, 1 - k)
    attend(y, z, True)
    plus(1)
    minus(1)
    cross(z)
    plus(2)
    visit(z - 1 >= 0, y, lo(1))
    minus(2)
    visit(z + 1 >= 8, y, hi(1))
    cross(lo(1))
    visit(y1, zero, z)
    cross(hi(1))
    plus(3)
    visit(z - 2 >= 0, y, lo(2))
    minus(3)
    visit(z + 2 >= 8, y, hi(2))
    cross(lo(2))
    visit(jnp.logical_and(y1, seen(lo(1))), zero, lo(1))
    cross(hi(2))
    visit(jnp.logical_and(y1, seen(hi(1))), zero, hi(1))
    plus(4)
    visit(z - 3 >= 0, y, lo(3))
    minus(4)
    visit(z + 3 >= 8, y, hi(3))
    cross(lo(3))
    visit(jnp.logical_and(y1, seen(lo(2))), zero, lo(2))
    cross(hi(3))
    visit(jnp.logical_and(y1, seen(hi(2))), zero, hi(2))
    visit(z + 4 >= 8, y, hi(4))
    visit(jnp.logical_and(y1, seen(lo(3))), zero, lo(3))
    cross(lo(4))
    visit(jnp.logical_and(y1, seen(hi(3))), zero, hi(3))
    visit(jnp.logical_and(y1, seen(lo(4))), zero, lo(4))

    gc = Gather(AT, H1, c_send, c_recv)
    for h in range(NH):
        o = ACC[h] / jnp.sum(L[h], axis=1, keepdims=True)
        AT[:, pl.ds(pl.multiple_of(tp * H1 + h * HD, 128), HD)] = o.astype(BF)
    gc.start()
    loads[3].wait()
    OACC[...] = G[:, own_cols].astype(F32)

    def project(xi):
        rows = pl.ds(pl.multiple_of(xi * 2 * H1, 128), 2 * H1)
        OACC[...] += jnp.dot(AT[:, rows], Wo[rows, :], preferred_element_type=F32)

    gc.pass_on(True)
    gc.rest()
    gc.pass_on(False)
    gc.part(0)
    gc.part(1)
    gc.across(True)
    gc.part(2)
    gc.part(3)
    gc.across(False)
    project(x)
    gc.wait(LEFT, 2, 3)
    gc.wait(RIGHT, 0, 1)
    gc.wait(PLEFT, 0, 1, 2, 3)
    gc.wait(PRIGHT, 0, 1, 2, 3)
    project(xl)
    project(xr)
    gc.wait(POPP, 0, 1, 2, 3)
    rows = pl.ds(pl.multiple_of(xo * 2 * H1, 128), 2 * H1)
    for i in (0, 2):
        part = pl.ds(i * (T // 4), T // 2)
        added = jnp.dot(AT[part, rows], Wo[rows, :], preferred_element_type=F32)
        MIX[part, :] = (OACC[part, :] + added).astype(BF)
        for c in written[2 + i:4 + i]:
            c.start()
    ga.drain()
    gc.drain()
    for c in written:
        c.wait()
    for cond, c in sent:
        if cond is None:
            c.wait_send()
        else:
            pl.when(cond)(c.wait_send)


def finish(a, b, c, oa, ob, oc, va, vb, vc, sems):
    parts = 4
    step = a.shape[0] // parts
    moves = [(b, vb, ob), (c, vc, oc)]
    moves += [tuple(r.at[pl.ds(i * step, step), :] for r in (a, va, oa)) for i in range(parts)]
    ins = [pltpu.make_async_copy(r, v, sems.at[i]) for i, (r, v, o) in enumerate(moves)]
    outs = [pltpu.make_async_copy(v, o, sems.at[len(moves) + i]) for i, (r, v, o) in enumerate(moves)]
    for cpy in ins:
        cpy.start()
    for c_in, c_out in zip(ins, outs):
        c_in.wait()
        c_out.start()
    for cpy in outs:
        cpy.wait()


def local(
    hidden_in, norm_gain, seq_lengths, w_query, b_query, w_key, b_key, w_value, b_value, w_out
):
    T, D1 = hidden_in.shape
    D = w_query.shape[0]
    H1 = w_query.shape[1]
    NH = H1 // HD
    f = (ROPE_BASE ** (-np.arange(HD // 2) / (HD // 2))).astype(np.float32)
    freq = jnp.asarray(np.concatenate([f, f]).reshape(1, HD))
    vm = pl.BlockSpec(memory_space=pltpu.VMEM)
    hb = pl.BlockSpec(memory_space=pl.ANY)
    V = pltpu.VMEM
    made = pl.pallas_call(
        kernel,
        out_shape=(
            jax.ShapeDtypeStruct((T, D1), BF),
            jax.ShapeDtypeStruct((T, HD), BF),
            jax.ShapeDtypeStruct((T, HD), BF),
        ),
        in_specs=[hb] * 11,
        out_specs=(hb, hb, hb),
        scratch_shapes=[
            V((1, D), F32), V((NH, HD), BF), V((1, HD), BF), V((1, HD), BF), V((1, HD), F32),
            pltpu.SMEM(seq_lengths.shape, jnp.int32),
            V((T, D), BF), V((T, D), BF), V((D, H1 + 2 * HD), BF), V(w_out.shape, BF),
            V((32, T, HD), BF), V((32, T, HD), BF), V((T, 8 * H1), BF), V((NH, T, HD), BF),
            V((NH, T, HD), F32), V((NH, T, HD), F32), V((NH, T, HD), F32),
            V((T, HD), F32), V((T, HD), F32), V((T, HD), BF), V((32, T, HD), BF), V((T, HD), F32),
            V((T, D1), F32), V((T, D1), BF),
            pltpu.SemaphoreType.DMA((21,)),
            pltpu.SemaphoreType.DMA((28,)), pltpu.SemaphoreType.DMA((32,)),
            pltpu.SemaphoreType.DMA((28,)), pltpu.SemaphoreType.DMA((32,)),
            pltpu.SemaphoreType.DMA((SENDS,)), pltpu.SemaphoreType.DMA((64,)),
        ],
        compiler_params=pltpu.CompilerParams(
            collective_id=0, has_side_effects=True, vmem_limit_bytes=60 * 1024 * 1024
        ),
        name="layer",
    )(
        hidden_in, norm_gain.reshape(1, D), seq_lengths, w_query, b_query.reshape(NH, HD),
        w_key, b_key.reshape(1, HD), w_value, b_value.reshape(1, HD), w_out, freq,
    )
    return pl.pallas_call(
        finish,
        out_shape=tuple(jax.ShapeDtypeStruct(m.shape, m.dtype) for m in made),
        in_specs=[hb, hb, hb],
        out_specs=(hb, hb, hb),
        scratch_shapes=[V(m.shape, m.dtype) for m in made] + [pltpu.SemaphoreType.DMA((12,))],
        name="finish",
    )(*made)


def solution(mesh):
    placed = (
        P("cp", "tp"), P(), P(), P(None, "tp"), P("tp"), P(None, "tp"), P("tp"),
        P(None, "tp"), P("tp"), P(None, "tp"),
    )
    return jax.shard_map(
        local, mesh=mesh, in_specs=placed,
        out_specs=(P("cp", "tp"), P("cp", "tp"), P("cp", "tp")), check_vma=False,
    )
```

```python
import jax
import jax.numpy as jnp
import numpy as np
from jax import lax
from jax.experimental import pallas as pl
from jax.experimental.pallas import tpu as pltpu
from jax.sharding import PartitionSpec as P

HD = 128
EPS = 1e-06
ROPE_BASE = 1000000.0
FAR = -float(2**100)
LOG2E = 1.4426950408889634
MESH = pl.DeviceIdType.MESH
BF = jnp.bfloat16
F32 = jnp.float32
LEFT, RIGHT, OPP, PART, PLEFT, PRIGHT, POPP = 1, 2, 3, 4, 5, 6, 7
SENDS = 72


def kernel(
    hid, gain_h, seq_h, wq, bq_h, wk, bk_h, wv, bv_h, wo, freq_h,
    mixed, kout, vout,
    gain, bq, bk, bv, freq, seq, G, N, W, Wo, Kb, Vb, AT, Q, M, L, ACC, COS, SIN, QDOC, DOC, SS, OACC, MIX,
    lsem, a_send, a_recv, c_send, c_recv, kv_send, kv_recv,
):
    T = hid.shape[0]
    D1 = hid.shape[1]
    H1 = wo.shape[0] // 8
    NH = H1 // HD
    cp = lax.axis_index("cp")
    tp = lax.axis_index("tp")
    y = lax.div(cp, 16)
    z = lax.div(lax.rem(cp, 16), 2)
    k = lax.rem(cp, 2)
    x = lax.div(tp, 2)
    yh = lax.rem(tp, 2)
    xl = lax.rem(x + 3, 4)
    xr = lax.rem(x + 1, 4)
    xo = lax.rem(x + 2, 4)
    right = (cp, 2 * xr + yh)
    left = (cp, 2 * xl + yh)
    partner = (cp, 2 * x + 1 - yh)
    zplus = (y * 16 + lax.rem(z + 1, 8) * 2 + k, tp)
    zminus = (y * 16 + lax.rem(z + 7, 8) * 2 + k, tp)
    ypart = ((1 - y) * 16 + z * 2 + k, tp)
    sib = (y * 16 + z * 2 + 1 - k, tp)
    diag = ((1 - y) * 16 + lax.rem(z + 1 + 6 * y, 8) * 2 + k, tp)

    own_cols = pl.ds(pl.multiple_of(tp * D1, 128), D1)
    quarters = [pl.ds(i * (T // 4), T // 4) for i in range(4)]
    load_hid = [
        pltpu.make_async_copy(hid.at[q, :], G.at[q, own_cols], lsem.at[11 + i]) for i, q in enumerate(quarters)
    ]
    for c in load_hid:
        c.start()
    loads = [
        pltpu.make_async_copy(wk, W.at[:, pl.ds(H1, HD)], lsem.at[1]),
        pltpu.make_async_copy(wv, W.at[:, pl.ds(H1 + HD, HD)], lsem.at[2]),
        pltpu.make_async_copy(wq, W.at[:, pl.ds(0, H1)], lsem.at[3]),
        pltpu.make_async_copy(wo, Wo, lsem.at[4]),
    ]
    small = [
        pltpu.make_async_copy(a, b, lsem.at[5 + i])
        for i, (a, b) in enumerate(
            ((seq_h, seq), (freq_h, freq), (gain_h, gain), (bq_h, bq), (bk_h, bk), (bv_h, bv))
        )
    ]

    written = [
        pltpu.make_async_copy(Kb.at[cp], kout, lsem.at[15]),
        pltpu.make_async_copy(Vb.at[cp], vout, lsem.at[16]),
    ] + [
        pltpu.make_async_copy(MIX.at[q, :], mixed.at[q, :], lsem.at[17 + i]) for i, q in enumerate(quarters)
    ]

    barrier = pltpu.get_barrier_semaphore()
    for dev in (right, left, partner, zplus, zminus, ypart, sib, diag):
        pl.semaphore_signal(barrier, inc=1, device_id=dev, device_id_type=MESH)
    for c in small + loads:
        c.start()
    pl.semaphore_wait(barrier, 8)
    for c in load_hid:
        c.wait()

    tps = {
        0: 2 * x + yh, LEFT: 2 * xl + yh, RIGHT: 2 * xr + yh, OPP: 2 * xo + yh,
        PART: 2 * x + 1 - yh, PLEFT: 2 * xl + 1 - yh, PRIGHT: 2 * xr + 1 - yh, POPP: 2 * xo + 1 - yh,
    }

    class Gather:
        def __init__(self, buf, width, ssem, rsem):
            self.buf, self.width, self.ssem, self.rsem = buf, width, ssem, rsem
            self.sent = []

        def ref(self, slot, c):
            cols = pl.ds(pl.multiple_of(tps[slot] * self.width, 128), self.width)
            return self.buf.at[pl.ds(c * (T // 4), T // 4), cols]

        def send(self, slot, c, dev, dst_slot):
            r = self.ref(slot, c)
            cpy = pltpu.make_async_remote_copy(
                src_ref=r, dst_ref=r, send_sem=self.ssem.at[len(self.sent)],
                recv_sem=self.rsem.at[dst_slot * 4 + c], device_id=dev, device_id_type=MESH,
            )
            cpy.start()
            self.sent.append(cpy)

        def wait(self, slot, *chunks):
            for c in chunks:
                r = self.ref(slot, c)
                pltpu.make_async_remote_copy(
                    src_ref=r, dst_ref=r, send_sem=self.ssem.at[0],
                    recv_sem=self.rsem.at[slot * 4 + c], device_id=right, device_id_type=MESH,
                ).wait_recv()

        def start(self):
            for c in (0, 1, 2):
                self.send(0, c, right, LEFT)
                self.send(0, (c + 2) % 4, left, RIGHT)
                self.send(0, c, partner, PART)
            self.send(0, 3, partner, PART)

        def pass_on(self, first):
            up, dn = (0, 2) if first else (1, 3)
            self.wait(LEFT, up)
            self.send(LEFT, up, right, OPP)
            self.wait(RIGHT, dn)
            self.send(RIGHT, dn, left, OPP)

        def rest(self):
            self.send(0, 3, right, LEFT)
            self.send(0, 1, left, RIGHT)

        def part(self, c):
            self.wait(PART, c)
            self.send(PART, c, right, PLEFT)
            self.send(PART, c, left, PRIGHT)

        def across(self, first):
            for c in ((0, 2) if first else (1, 3)):
                self.wait(OPP, c)
                self.send(OPP, c, partner, POPP)

        def drain(self):
            for c in self.sent:
                c.wait_send()

    ga = Gather(G, D1, a_send, a_recv)
    ga.start()

    for c in small:
        c.wait()

    lane = lax.broadcasted_iota(jnp.int32, (1, HD), 1)
    starts = jnp.full((1, HD), 1 << 30, jnp.int32)
    ends = jnp.zeros((1, HD), jnp.int32)
    tok = lax.broadcasted_iota(jnp.int32, (T, HD), 0) + cp * T
    first = jnp.zeros((T, HD), jnp.int32)
    edge = jnp.int32(0)
    for j in range(seq.shape[0]):
        first = jnp.where(tok >= edge, edge, first)
        starts = jnp.where(lane == j, edge, starts)
        edge = edge + seq[j]
        ends = jnp.where(lane == j, edge, ends)
    angle = (tok - first).astype(F32) * freq[...]
    COS[...] = jnp.cos(angle)
    sgn = jnp.where(lax.broadcasted_iota(jnp.int32, (T, HD), 1) < HD // 2, -1.0, 1.0)
    SIN[...] = jnp.sin(angle) * sgn
    inside = jnp.logical_and(tok >= starts, tok < ends)
    QDOC[...] = jnp.where(inside, FAR, 0.0).astype(BF)
    live = lane < seq.shape[0]

    def doc_block(i, carry):
        pos = lax.broadcasted_iota(jnp.int32, (T, HD), 0) + i * T
        out = jnp.logical_or(pos < starts, pos >= ends)
        DOC[i] = jnp.where(jnp.logical_and(out, live), 1.0, 0.0).astype(BF)
        return carry

    lax.fori_loop(0, DOC.shape[0], doc_block, 0)

    def slab(slot):
        return pl.ds(pl.multiple_of(tps[slot] * D1, 128), D1)

    def squares(slots, init=False):
        total = None if init else SS[...]
        for s in slots:
            v = G[:, slab(s)].astype(F32)
            v = v * v
            for c in range(D1 // HD):
                piece = v[:, c * HD:(c + 1) * HD]
                total = piece if total is None else total + piece
        SS[...] = total

    def rope(u):
        return u * COS[...] + pltpu.roll(u, HD // 2, 1) * SIN[...]

    def keys_values():
        inv = lax.rsqrt(jnp.sum(SS[...], axis=1, keepdims=True) / (8.0 * D1) + EPS)
        pair = 2 * D1
        kv = None
        for i in range(4):
            sl = slice(i * pair, (i + 1) * pair)
            n = (G[:, sl].astype(F32) * inv * gain[:, sl]).astype(BF)
            N[:, sl] = n
            part = jnp.dot(n, W[sl, H1:], preferred_element_type=F32)
            kv = part if kv is None else kv + part
        knew = rope(kv[:, :HD] + bk[...].astype(F32)).astype(BF)
        vnew = (kv[:, HD:] + bv[...].astype(F32)).astype(BF)
        Kb[cp] = knew
        Vb[cp] = vnew
        for c in written[:2]:
            c.start()

    def queries():
        q = jnp.dot(N[...], W[:, :H1], preferred_element_type=F32)
        for h in range(NH):
            Q[h] = rope(q[:, h * HD:(h + 1) * HD] + bq[h:h + 1, :].astype(F32)).astype(BF)

    sent = []

    def piece(part, p, s, kk):
        blk = p * 16 + s * 2 + kk
        return (Kb if part == 0 else Vb).at[blk], kv_recv.at[part * 32 + blk]

    def send(cond, part, p, s, dev):
        r, rs = piece(part, p, s, k)
        c = pltpu.make_async_remote_copy(
            src_ref=r, dst_ref=r, send_sem=kv_send.at[len(sent)], recv_sem=rs,
            device_id=dev, device_id_type=MESH,
        )
        if cond is None:
            c.start()
        else:
            pl.when(cond)(c.start)
        sent.append((cond, c))

    def wait_for(cond, part, p, s, kk):
        r, rs = piece(part, p, s, kk)
        c = pltpu.make_async_remote_copy(
            src_ref=r, dst_ref=r, send_sem=kv_send.at[0], recv_sem=rs,
            device_id=sib, device_id_type=MESH,
        )
        if cond is None:
            c.wait_recv()
        else:
            pl.when(cond)(c.wait_recv)

    scale = HD ** (-0.5) * LOG2E

    def attend(p, s, diag):
        b0 = p * 16 + s * 2
        keys = jnp.concatenate(
            [Kb[pl.ds(b0, 2)].reshape(2 * T, HD), DOC[pl.ds(b0, 2)].reshape(2 * T, HD)], axis=1
        )
        vals = Vb[pl.ds(b0, 2)].reshape(2 * T, HD)
        qs = jnp.concatenate([jnp.concatenate([Q[h], QDOC[...]], axis=1) for h in range(NH)], axis=0)
        sc = lax.dot_general(qs, keys, (((1,), (1,)), ((), ())), preferred_element_type=F32)
        if diag:
            kpos = lax.broadcasted_iota(jnp.int32, (T, 2 * T), 1)
            qpos = lax.broadcasted_iota(jnp.int32, (T, 2 * T), 0) + k * T
            sc = jnp.concatenate([jnp.where(kpos <= qpos, sc[h * T:(h + 1) * T], FAR) for h in range(NH)], axis=0)
        top = jnp.max(sc, axis=1, keepdims=True)
        m_old = M[...].reshape(NH * T, HD)
        if not diag:
            top = jnp.maximum(top, m_old[:, :1])
        w = jnp.exp2((sc - top) * scale)
        tot = w[:, :HD]
        for c in range(1, 2 * T // HD):
            tot = tot + w[:, c * HD:(c + 1) * HD]
        add = jnp.dot(w.astype(BF), vals, preferred_element_type=F32)
        if not diag:
            f = jnp.exp2((m_old - top) * scale)
            tot = L[...].reshape(NH * T, HD) * f + tot
            add = ACC[...].reshape(NH * T, HD) * f + add
        L[...] = tot.reshape(NH, T, HD)
        ACC[...] = add.reshape(NH, T, HD)
        M[...] = jnp.broadcast_to(top, (NH * T, HD)).reshape(NH, T, HD)

    y0 = y == 0
    y1 = y == 1
    zero = jnp.int32(0)
    KINDS = (("KO", 0, y), ("VO", 1, y), ("KX", 0, zero))

    def up(kind, s, d):
        low = s + d <= 7
        if kind == "KX":
            return y1 if d <= 4 else None
        if kind == "KO":
            return low if d <= 3 else None
        return jnp.logical_or(y0, low) if d <= 3 else (jnp.logical_and(y0, low) if d == 4 else None)

    def down(kind, s, d):
        if kind == "KX":
            return jnp.logical_and(y1, s - d >= 0) if d <= 3 else None
        if kind == "KO":
            return s <= 3 if d <= 4 else None
        return jnp.logical_or(y0, s <= 3) if d <= 3 else (jnp.logical_and(y1, s <= 3) if d == 4 else None)

    def seen(s):
        return s >= z - 4

    def own():
        for part in (0, 1):
            kind = ("KO", "VO")[part]
            send(up(kind, z, 1), part, y, z, zplus)
            send(down(kind, z, 1), part, y, z, zminus)
            if part == 0:
                send(y0, part, y, z, diag)
            send(y0, part, y, z, ypart)
            send(None, part, y, z, sib)

    def first_key():
        wait_for(y1, 0, zero, z, k)
        send(down("KX", z, 1), 0, zero, z, zminus)
        send(y1, 0, zero, z, sib)

    def hop(d, step, go, dev, mine):
        s = lax.rem(z + 8 + step * d, 8)
        for kind, part, p in KINDS:
            got = go(kind, s, d)
            if got is None:
                continue
            wait_for(got, part, p, s, k)
            on = go(kind, s, d + 1)
            if on is not None:
                send(on, part, p, s, dev)
            if kind == "VO" and step < 0 and d == 3:
                send(y0, part, p, s, diag)
            if kind == "VO" and d <= 3:
                send(jnp.logical_and(y0, seen(s)), part, p, s, ypart)
            send(got if kind == "KX" else jnp.logical_and(got, mine), part, p, s, sib)

    def plus(d):
        hop(d, -1, up, zplus, z - d >= 0)

    def minus(d):
        hop(d, 1, down, zminus, z + d >= 8)

    def cross(s):
        here = jnp.logical_and(y1, seen(s))
        wait_for(here, 1, zero, s, k)
        send(here, 1, zero, s, sib)

    def lo(d):
        return lax.rem(z + 8 - d, 8)

    def hi(d):
        return lax.rem(z + d, 8)

    def visit(cond, p, s):
        @pl.when(cond)
        def _():
            wait_for(None, 0, p, s, 1 - k)
            wait_for(None, 1, p, s, 1 - k)
            attend(p, s, False)

    ga.pass_on(True)
    ga.rest()
    squares((0,), True)
    ga.pass_on(False)
    ga.part(0)
    ga.part(1)
    ga.across(True)
    ga.part(2)
    ga.part(3)
    ga.wait(LEFT, 2, 3)
    ga.wait(RIGHT, 0, 1)
    squares((LEFT, RIGHT))
    ga.across(False)
    squares((PART, OPP))
    ga.wait(PLEFT, 0, 1, 2, 3)
    ga.wait(PRIGHT, 0, 1, 2, 3)
    squares((PLEFT, PRIGHT))
    ga.wait(POPP, 0, 1, 2, 3)
    squares((POPP,))
    loads[0].wait()
    loads[1].wait()
    keys_values()
    own()
    loads[2].wait()
    queries()
    first_key()
    wait_for(None, 0, y, z, 1 - k)
    wait_for(None, 1, y, z, 1 - k)
    attend(y, z, True)
    plus(1)
    minus(1)
    cross(z)
    plus(2)
    visit(z - 1 >= 0, y, lo(1))
    minus(2)
    visit(z + 1 >= 8, y, hi(1))
    cross(lo(1))
    visit(y1, zero, z)
    cross(hi(1))
    plus(3)
    visit(z - 2 >= 0, y, lo(2))
    minus(3)
    visit(z + 2 >= 8, y, hi(2))
    cross(lo(2))
    visit(jnp.logical_and(y1, seen(lo(1))), zero, lo(1))
    cross(hi(2))
    visit(jnp.logical_and(y1, seen(hi(1))), zero, hi(1))
    plus(4)
    visit(z - 3 >= 0, y, lo(3))
    minus(4)
    visit(z + 3 >= 8, y, hi(3))
    cross(lo(3))
    visit(jnp.logical_and(y1, seen(lo(2))), zero, lo(2))
    cross(hi(3))
    visit(jnp.logical_and(y1, seen(hi(2))), zero, hi(2))
    cross(lo(4))
    visit(z + 4 >= 8, y, hi(4))
    visit(jnp.logical_and(y1, seen(lo(3))), zero, lo(3))
    visit(jnp.logical_and(y1, seen(hi(3))), zero, hi(3))
    visit(jnp.logical_and(y1, seen(lo(4))), zero, lo(4))

    gc = Gather(AT, H1, c_send, c_recv)
    for h in range(NH):
        o = ACC[h] / jnp.sum(L[h], axis=1, keepdims=True)
        AT[:, pl.ds(pl.multiple_of(tp * H1 + h * HD, 128), HD)] = o.astype(BF)
    gc.start()
    loads[3].wait()
    OACC[...] = G[:, own_cols].astype(F32)

    def project(xi):
        rows = pl.ds(pl.multiple_of(xi * 2 * H1, 128), 2 * H1)
        OACC[...] += jnp.dot(AT[:, rows], Wo[rows, :], preferred_element_type=F32)

    gc.pass_on(True)
    gc.rest()
    gc.pass_on(False)
    gc.part(0)
    gc.part(1)
    gc.across(True)
    gc.part(2)
    gc.part(3)
    gc.across(False)
    project(x)
    gc.wait(LEFT, 2, 3)
    gc.wait(RIGHT, 0, 1)
    gc.wait(PLEFT, 0, 1, 2, 3)
    gc.wait(PRIGHT, 0, 1, 2, 3)
    project(xl)
    project(xr)
    gc.wait(POPP, 0, 1, 2, 3)
    rows = pl.ds(pl.multiple_of(xo * 2 * H1, 128), 2 * H1)
    for i in (0, 2):
        part = pl.ds(i * (T // 4), T // 2)
        added = jnp.dot(AT[part, rows], Wo[rows, :], preferred_element_type=F32)
        MIX[part, :] = (OACC[part, :] + added).astype(BF)
        for c in written[2 + i:4 + i]:
            c.start()
    ga.drain()
    gc.drain()
    for c in written:
        c.wait()
    for cond, c in sent:
        if cond is None:
            c.wait_send()
        else:
            pl.when(cond)(c.wait_send)


def finish(a, b, c, oa, ob, oc, va, vb, vc, sems):
    parts = 4
    step = a.shape[0] // parts
    moves = [(b, vb, ob), (c, vc, oc)]
    moves += [tuple(r.at[pl.ds(i * step, step), :] for r in (a, va, oa)) for i in range(parts)]
    ins = [pltpu.make_async_copy(r, v, sems.at[i]) for i, (r, v, o) in enumerate(moves)]
    outs = [pltpu.make_async_copy(v, o, sems.at[len(moves) + i]) for i, (r, v, o) in enumerate(moves)]
    for cpy in ins:
        cpy.start()
    for c_in, c_out in zip(ins, outs):
        c_in.wait()
        c_out.start()
    for cpy in outs:
        cpy.wait()


def local(
    hidden_in, norm_gain, seq_lengths, w_query, b_query, w_key, b_key, w_value, b_value, w_out
):
    T, D1 = hidden_in.shape
    D = w_query.shape[0]
    H1 = w_query.shape[1]
    NH = H1 // HD
    f = (ROPE_BASE ** (-np.arange(HD // 2) / (HD // 2))).astype(np.float32)
    freq = jnp.asarray(np.concatenate([f, f]).reshape(1, HD))
    vm = pl.BlockSpec(memory_space=pltpu.VMEM)
    hb = pl.BlockSpec(memory_space=pl.ANY)
    V = pltpu.VMEM
    made = pl.pallas_call(
        kernel,
        out_shape=(
            jax.ShapeDtypeStruct((T, D1), BF),
            jax.ShapeDtypeStruct((T, HD), BF),
            jax.ShapeDtypeStruct((T, HD), BF),
        ),
        in_specs=[hb] * 11,
        out_specs=(hb, hb, hb),
        scratch_shapes=[
            V((1, D), F32), V((NH, HD), BF), V((1, HD), BF), V((1, HD), BF), V((1, HD), F32),
            pltpu.SMEM(seq_lengths.shape, jnp.int32),
            V((T, D), BF), V((T, D), BF), V((D, H1 + 2 * HD), BF), V(w_out.shape, BF),
            V((32, T, HD), BF), V((32, T, HD), BF), V((T, 8 * H1), BF), V((NH, T, HD), BF),
            V((NH, T, HD), F32), V((NH, T, HD), F32), V((NH, T, HD), F32),
            V((T, HD), F32), V((T, HD), F32), V((T, HD), BF), V((32, T, HD), BF), V((T, HD), F32),
            V((T, D1), F32), V((T, D1), BF),
            pltpu.SemaphoreType.DMA((21,)),
            pltpu.SemaphoreType.DMA((28,)), pltpu.SemaphoreType.DMA((32,)),
            pltpu.SemaphoreType.DMA((28,)), pltpu.SemaphoreType.DMA((32,)),
            pltpu.SemaphoreType.DMA((SENDS,)), pltpu.SemaphoreType.DMA((64,)),
        ],
        compiler_params=pltpu.CompilerParams(
            collective_id=0, has_side_effects=True, vmem_limit_bytes=60 * 1024 * 1024
        ),
        name="layer",
    )(
        hidden_in, norm_gain.reshape(1, D), seq_lengths, w_query, b_query.reshape(NH, HD),
        w_key, b_key.reshape(1, HD), w_value, b_value.reshape(1, HD), w_out, freq,
    )
    return pl.pallas_call(
        finish,
        out_shape=tuple(jax.ShapeDtypeStruct(m.shape, m.dtype) for m in made),
        in_specs=[hb, hb, hb],
        out_specs=(hb, hb, hb),
        scratch_shapes=[V(m.shape, m.dtype) for m in made] + [pltpu.SemaphoreType.DMA((12,))],
        name="finish",
    )(*made)


def solution(mesh):
    placed = (
        P("cp", "tp"), P(), P(), P(None, "tp"), P("tp"), P(None, "tp"), P("tp"),
        P(None, "tp"), P("tp"), P(None, "tp"),
    )
    return jax.shard_map(
        local, mesh=mesh, in_specs=placed,
        out_specs=(P("cp", "tp"), P("cp", "tp"), P("cp", "tp")), check_vma=False,
    )
```

```python
import jax
import jax.numpy as jnp
import numpy as np
from jax import lax
from jax.experimental import pallas as pl
from jax.experimental.pallas import tpu as pltpu
from jax.sharding import PartitionSpec as P

HD = 128
EPS = 1e-06
ROPE_BASE = 1000000.0
FAR = -float(2**100)
LOG2E = 1.4426950408889634
MESH = pl.DeviceIdType.MESH
BF = jnp.bfloat16
F32 = jnp.float32
LEFT, RIGHT, OPP, PART, PLEFT, PRIGHT, POPP = 1, 2, 3, 4, 5, 6, 7
SENDS = 72


def kernel(
    hid, gain_h, seq_h, wq, bq_h, wk, bk_h, wv, bv_h, wo, freq_h,
    mixed, kout, vout,
    gain, bq, bk, bv, freq, seq, G, N, W, Wo, Kb, Vb, AT, Q, M, L, ACC, COS, SIN, QDOC, DOC, SS, OACC, MIX,
    lsem, a_send, a_recv, c_send, c_recv, kv_send, kv_recv,
):
    T = hid.shape[0]
    D1 = hid.shape[1]
    H1 = wo.shape[0] // 8
    NH = H1 // HD
    cp = lax.axis_index("cp")
    tp = lax.axis_index("tp")
    y = lax.div(cp, 16)
    z = lax.div(lax.rem(cp, 16), 2)
    k = lax.rem(cp, 2)
    x = lax.div(tp, 2)
    yh = lax.rem(tp, 2)
    xl = lax.rem(x + 3, 4)
    xr = lax.rem(x + 1, 4)
    xo = lax.rem(x + 2, 4)
    right = (cp, 2 * xr + yh)
    left = (cp, 2 * xl + yh)
    partner = (cp, 2 * x + 1 - yh)
    zplus = (y * 16 + lax.rem(z + 1, 8) * 2 + k, tp)
    zminus = (y * 16 + lax.rem(z + 7, 8) * 2 + k, tp)
    ypart = ((1 - y) * 16 + z * 2 + k, tp)
    sib = (y * 16 + z * 2 + 1 - k, tp)
    diag = ((1 - y) * 16 + lax.rem(z + 1 + 6 * y, 8) * 2 + k, tp)

    own_cols = pl.ds(pl.multiple_of(tp * D1, 128), D1)
    quarters = [pl.ds(i * (T // 4), T // 4) for i in range(4)]
    load_hid = [
        pltpu.make_async_copy(hid.at[q, :], G.at[q, own_cols], lsem.at[11 + i]) for i, q in enumerate(quarters)
    ]
    for c in load_hid:
        c.start()
    loads = [
        pltpu.make_async_copy(wk, W.at[:, pl.ds(H1, HD)], lsem.at[1]),
        pltpu.make_async_copy(wv, W.at[:, pl.ds(H1 + HD, HD)], lsem.at[2]),
        pltpu.make_async_copy(wq, W.at[:, pl.ds(0, H1)], lsem.at[3]),
        pltpu.make_async_copy(wo, Wo, lsem.at[4]),
    ]
    small = [
        pltpu.make_async_copy(a, b, lsem.at[5 + i])
        for i, (a, b) in enumerate(
            ((seq_h, seq), (freq_h, freq), (gain_h, gain), (bq_h, bq), (bk_h, bk), (bv_h, bv))
        )
    ]

    written = [
        pltpu.make_async_copy(Kb.at[cp], kout, lsem.at[15]),
        pltpu.make_async_copy(Vb.at[cp], vout, lsem.at[16]),
    ] + [
        pltpu.make_async_copy(MIX.at[q, :], mixed.at[q, :], lsem.at[17 + i]) for i, q in enumerate(quarters)
    ]

    barrier = pltpu.get_barrier_semaphore()
    for dev in (right, left, partner, zplus, zminus, ypart, sib, diag):
        pl.semaphore_signal(barrier, inc=1, device_id=dev, device_id_type=MESH)
    for c in small + loads:
        c.start()
    pl.semaphore_wait(barrier, 8)
    for c in load_hid:
        c.wait()

    tps = {
        0: 2 * x + yh, LEFT: 2 * xl + yh, RIGHT: 2 * xr + yh, OPP: 2 * xo + yh,
        PART: 2 * x + 1 - yh, PLEFT: 2 * xl + 1 - yh, PRIGHT: 2 * xr + 1 - yh, POPP: 2 * xo + 1 - yh,
    }

    class Gather:
        def __init__(self, buf, width, ssem, rsem):
            self.buf, self.width, self.ssem, self.rsem = buf, width, ssem, rsem
            self.sent = []

        def ref(self, slot, c):
            cols = pl.ds(pl.multiple_of(tps[slot] * self.width, 128), self.width)
            return self.buf.at[pl.ds(c * (T // 4), T // 4), cols]

        def send(self, slot, c, dev, dst_slot):
            r = self.ref(slot, c)
            cpy = pltpu.make_async_remote_copy(
                src_ref=r, dst_ref=r, send_sem=self.ssem.at[len(self.sent)],
                recv_sem=self.rsem.at[dst_slot * 4 + c], device_id=dev, device_id_type=MESH,
            )
            cpy.start()
            self.sent.append(cpy)

        def wait(self, slot, *chunks):
            for c in chunks:
                r = self.ref(slot, c)
                pltpu.make_async_remote_copy(
                    src_ref=r, dst_ref=r, send_sem=self.ssem.at[0],
                    recv_sem=self.rsem.at[slot * 4 + c], device_id=right, device_id_type=MESH,
                ).wait_recv()

        def start(self):
            for c in (0, 1, 2):
                self.send(0, c, right, LEFT)
                self.send(0, (c + 2) % 4, left, RIGHT)
                self.send(0, c, partner, PART)
            self.send(0, 3, partner, PART)

        def pass_on(self, first):
            up, dn = (0, 2) if first else (1, 3)
            self.wait(LEFT, up)
            self.send(LEFT, up, right, OPP)
            self.wait(RIGHT, dn)
            self.send(RIGHT, dn, left, OPP)

        def rest(self):
            self.send(0, 3, right, LEFT)
            self.send(0, 1, left, RIGHT)

        def part(self, c):
            self.wait(PART, c)
            self.send(PART, c, right, PLEFT)
            self.send(PART, c, left, PRIGHT)

        def across(self, first):
            for c in ((0, 2) if first else (1, 3)):
                self.wait(OPP, c)
                self.send(OPP, c, partner, POPP)

        def drain(self):
            for c in self.sent:
                c.wait_send()

    ga = Gather(G, D1, a_send, a_recv)
    ga.start()

    for c in small:
        c.wait()

    lane = lax.broadcasted_iota(jnp.int32, (1, HD), 1)
    starts = jnp.full((1, HD), 1 << 30, jnp.int32)
    ends = jnp.zeros((1, HD), jnp.int32)
    tok = lax.broadcasted_iota(jnp.int32, (T, HD), 0) + cp * T
    first = jnp.zeros((T, HD), jnp.int32)
    edge = jnp.int32(0)
    for j in range(seq.shape[0]):
        first = jnp.where(tok >= edge, edge, first)
        starts = jnp.where(lane == j, edge, starts)
        edge = edge + seq[j]
        ends = jnp.where(lane == j, edge, ends)
    angle = (tok - first).astype(F32) * freq[...]
    COS[...] = jnp.cos(angle)
    sgn = jnp.where(lax.broadcasted_iota(jnp.int32, (T, HD), 1) < HD // 2, -1.0, 1.0)
    SIN[...] = jnp.sin(angle) * sgn
    inside = jnp.logical_and(tok >= starts, tok < ends)
    QDOC[...] = jnp.where(inside, FAR, 0.0).astype(BF)
    live = lane < seq.shape[0]

    def doc_block(i, carry):
        pos = lax.broadcasted_iota(jnp.int32, (T, HD), 0) + i * T
        out = jnp.logical_or(pos < starts, pos >= ends)
        DOC[i] = jnp.where(jnp.logical_and(out, live), 1.0, 0.0).astype(BF)
        return carry

    lax.fori_loop(0, DOC.shape[0], doc_block, 0)

    def slab(slot):
        return pl.ds(pl.multiple_of(tps[slot] * D1, 128), D1)

    def squares(slots, init=False):
        total = None if init else SS[...]
        for s in slots:
            v = G[:, slab(s)].astype(F32)
            v = v * v
            for c in range(D1 // HD):
                piece = v[:, c * HD:(c + 1) * HD]
                total = piece if total is None else total + piece
        SS[...] = total

    def rope(u):
        return u * COS[...] + pltpu.roll(u, HD // 2, 1) * SIN[...]

    def keys_values():
        inv = lax.rsqrt(jnp.sum(SS[...], axis=1, keepdims=True) / (8.0 * D1) + EPS)
        pair = 2 * D1
        kv = None
        for i in range(4):
            sl = slice(i * pair, (i + 1) * pair)
            n = (G[:, sl].astype(F32) * inv * gain[:, sl]).astype(BF)
            N[:, sl] = n
            part = jnp.dot(n, W[sl, H1:], preferred_element_type=F32)
            kv = part if kv is None else kv + part
        knew = rope(kv[:, :HD] + bk[...].astype(F32)).astype(BF)
        vnew = (kv[:, HD:] + bv[...].astype(F32)).astype(BF)
        Kb[cp] = knew
        Vb[cp] = vnew
        for c in written[:2]:
            c.start()

    def queries():
        q = jnp.dot(N[...], W[:, :H1], preferred_element_type=F32)
        for h in range(NH):
            Q[h] = rope(q[:, h * HD:(h + 1) * HD] + bq[h:h + 1, :].astype(F32)).astype(BF)

    sent = []

    def piece(part, p, s, kk):
        blk = p * 16 + s * 2 + kk
        return (Kb if part == 0 else Vb).at[blk], kv_recv.at[part * 32 + blk]

    def send(cond, part, p, s, dev):
        r, rs = piece(part, p, s, k)
        c = pltpu.make_async_remote_copy(
            src_ref=r, dst_ref=r, send_sem=kv_send.at[len(sent)], recv_sem=rs,
            device_id=dev, device_id_type=MESH,
        )
        if cond is None:
            c.start()
        else:
            pl.when(cond)(c.start)
        sent.append((cond, c))

    def wait_for(cond, part, p, s, kk):
        r, rs = piece(part, p, s, kk)
        c = pltpu.make_async_remote_copy(
            src_ref=r, dst_ref=r, send_sem=kv_send.at[0], recv_sem=rs,
            device_id=sib, device_id_type=MESH,
        )
        if cond is None:
            c.wait_recv()
        else:
            pl.when(cond)(c.wait_recv)

    scale = HD ** (-0.5) * LOG2E

    def attend(p, s, diag):
        b0 = p * 16 + s * 2
        keys = jnp.concatenate(
            [Kb[pl.ds(b0, 2)].reshape(2 * T, HD), DOC[pl.ds(b0, 2)].reshape(2 * T, HD)], axis=1
        )
        vals = Vb[pl.ds(b0, 2)].reshape(2 * T, HD)
        qs = jnp.concatenate([jnp.concatenate([Q[h], QDOC[...]], axis=1) for h in range(NH)], axis=0)
        sc = lax.dot_general(qs, keys, (((1,), (1,)), ((), ())), preferred_element_type=F32)
        if diag:
            kpos = lax.broadcasted_iota(jnp.int32, (T, 2 * T), 1)
            qpos = lax.broadcasted_iota(jnp.int32, (T, 2 * T), 0) + k * T
            sc = jnp.concatenate([jnp.where(kpos <= qpos, sc[h * T:(h + 1) * T], FAR) for h in range(NH)], axis=0)
        top = jnp.max(sc, axis=1, keepdims=True)
        m_old = M[...].reshape(NH * T, HD)
        if not diag:
            top = jnp.maximum(top, m_old[:, :1])
        w = jnp.exp2((sc - top) * scale)
        tot = w[:, :HD]
        for c in range(1, 2 * T // HD):
            tot = tot + w[:, c * HD:(c + 1) * HD]
        add = jnp.dot(w.astype(BF), vals, preferred_element_type=F32)
        if not diag:
            f = jnp.exp2((m_old - top) * scale)
            tot = L[...].reshape(NH * T, HD) * f + tot
            add = ACC[...].reshape(NH * T, HD) * f + add
        L[...] = tot.reshape(NH, T, HD)
        ACC[...] = add.reshape(NH, T, HD)
        M[...] = jnp.broadcast_to(top, (NH * T, HD)).reshape(NH, T, HD)

    y0 = y == 0
    y1 = y == 1
    zero = jnp.int32(0)
    KINDS = (("KO", 0, y), ("VO", 1, y), ("KX", 0, zero))

    def up(kind, s, d):
        low = s + d <= 7
        if kind == "KX":
            return y1 if d <= 4 else None
        if kind == "KO":
            return low if d <= 3 else None
        return jnp.logical_or(y0, low) if d <= 3 else (jnp.logical_and(y0, low) if d == 4 else None)

    def down(kind, s, d):
        if kind == "KX":
            return jnp.logical_and(y1, s - d >= 0) if d <= 3 else None
        if kind == "KO":
            return s <= 3 if d <= 4 else None
        return jnp.logical_or(y0, s <= 3) if d <= 3 else (jnp.logical_and(y1, s <= 3) if d == 4 else None)

    def seen(s):
        return s >= z - 4

    def own():
        for part in (0, 1):
            kind = ("KO", "VO")[part]
            send(up(kind, z, 1), part, y, z, zplus)
            send(down(kind, z, 1), part, y, z, zminus)
            if part == 0:
                send(y0, part, y, z, diag)
            send(y0, part, y, z, ypart)
            send(None, part, y, z, sib)

    def first_key():
        wait_for(y1, 0, zero, z, k)
        send(down("KX", z, 1), 0, zero, z, zminus)
        send(y1, 0, zero, z, sib)

    def hop(d, step, go, dev, mine):
        s = lax.rem(z + 8 + step * d, 8)
        for kind, part, p in KINDS:
            got = go(kind, s, d)
            if got is None:
                continue
            wait_for(got, part, p, s, k)
            on = go(kind, s, d + 1)
            if on is not None:
                send(on, part, p, s, dev)
            if kind == "VO" and step < 0 and d == 3:
                send(y0, part, p, s, diag)
            if kind == "VO" and d <= 3:
                send(jnp.logical_and(y0, seen(s)), part, p, s, ypart)
            send(got if kind == "KX" else jnp.logical_and(got, mine), part, p, s, sib)

    def plus(d):
        hop(d, -1, up, zplus, z - d >= 0)

    def minus(d):
        hop(d, 1, down, zminus, z + d >= 8)

    def cross(s):
        here = jnp.logical_and(y1, seen(s))
        wait_for(here, 1, zero, s, k)
        send(here, 1, zero, s, sib)

    def lo(d):
        return lax.rem(z + 8 - d, 8)

    def hi(d):
        return lax.rem(z + d, 8)

    def visit(cond, p, s):
        @pl.when(cond)
        def _():
            wait_for(None, 0, p, s, 1 - k)
            wait_for(None, 1, p, s, 1 - k)
            attend(p, s, False)

    ga.pass_on(True)
    ga.rest()
    squares((0,), True)
    ga.pass_on(False)
    ga.part(0)
    ga.part(1)
    ga.across(True)
    ga.part(2)
    ga.part(3)
    ga.wait(LEFT, 2, 3)
    ga.wait(RIGHT, 0, 1)
    squares((LEFT, RIGHT))
    ga.across(False)
    squares((PART, OPP))
    ga.wait(PLEFT, 0, 1, 2, 3)
    ga.wait(PRIGHT, 0, 1, 2, 3)
    squares((PLEFT, PRIGHT))
    ga.wait(POPP, 0, 1, 2, 3)
    squares((POPP,))
    loads[0].wait()
    loads[1].wait()
    keys_values()
    own()
    loads[2].wait()
    queries()
    first_key()
    plus(1)
    minus(1)
    wait_for(None, 0, y, z, 1 - k)
    wait_for(None, 1, y, z, 1 - k)
    attend(y, z, True)
    cross(z)
    plus(2)
    visit(z - 1 >= 0, y, lo(1))
    minus(2)
    visit(z + 1 >= 8, y, hi(1))
    cross(lo(1))
    visit(y1, zero, z)
    cross(hi(1))
    plus(3)
    visit(z - 2 >= 0, y, lo(2))
    minus(3)
    visit(z + 2 >= 8, y, hi(2))
    cross(lo(2))
    visit(jnp.logical_and(y1, seen(lo(1))), zero, lo(1))
    cross(hi(2))
    visit(jnp.logical_and(y1, seen(hi(1))), zero, hi(1))
    plus(4)
    visit(z - 3 >= 0, y, lo(3))
    minus(4)
    visit(z + 3 >= 8, y, hi(3))
    cross(lo(3))
    visit(jnp.logical_and(y1, seen(lo(2))), zero, lo(2))
    cross(hi(3))
    visit(jnp.logical_and(y1, seen(hi(2))), zero, hi(2))
    cross(lo(4))
    visit(z + 4 >= 8, y, hi(4))
    visit(jnp.logical_and(y1, seen(lo(3))), zero, lo(3))
    visit(jnp.logical_and(y1, seen(hi(3))), zero, hi(3))
    visit(jnp.logical_and(y1, seen(lo(4))), zero, lo(4))

    gc = Gather(AT, H1, c_send, c_recv)
    def settle(c):
        rows = pl.ds(c * (T // 4), T // 4)
        for h in range(NH):
            o = ACC[h, rows, :] / jnp.sum(L[h, rows, :], axis=1, keepdims=True)
            AT[rows, pl.ds(pl.multiple_of(tp * H1 + h * HD, 128), HD)] = o.astype(BF)

    settle(0)
    settle(2)
    gc.send(0, 0, right, LEFT)
    gc.send(0, 2, left, RIGHT)
    gc.send(0, 0, partner, PART)
    settle(1)
    settle(3)
    gc.send(0, 1, right, LEFT)
    gc.send(0, 3, left, RIGHT)
    gc.send(0, 1, partner, PART)
    gc.send(0, 2, right, LEFT)
    gc.send(0, 0, left, RIGHT)
    gc.send(0, 2, partner, PART)
    gc.send(0, 3, partner, PART)
    loads[3].wait()
    OACC[...] = G[:, own_cols].astype(F32)

    def project(xi):
        rows = pl.ds(pl.multiple_of(xi * 2 * H1, 128), 2 * H1)
        OACC[...] += jnp.dot(AT[:, rows], Wo[rows, :], preferred_element_type=F32)

    gc.pass_on(True)
    gc.rest()
    gc.pass_on(False)
    gc.part(0)
    gc.part(1)
    gc.across(True)
    gc.part(2)
    gc.part(3)
    gc.across(False)
    project(x)
    gc.wait(LEFT, 2, 3)
    gc.wait(RIGHT, 0, 1)
    gc.wait(PLEFT, 0, 1, 2, 3)
    gc.wait(PRIGHT, 0, 1, 2, 3)
    project(xl)
    project(xr)
    gc.wait(POPP, 0, 1, 2, 3)
    rows = pl.ds(pl.multiple_of(xo * 2 * H1, 128), 2 * H1)
    for i in (0, 2):
        part = pl.ds(i * (T // 4), T // 2)
        added = jnp.dot(AT[part, rows], Wo[rows, :], preferred_element_type=F32)
        MIX[part, :] = (OACC[part, :] + added).astype(BF)
        for c in written[2 + i:4 + i]:
            c.start()
    ga.drain()
    gc.drain()
    for c in written:
        c.wait()
    for cond, c in sent:
        if cond is None:
            c.wait_send()
        else:
            pl.when(cond)(c.wait_send)


def finish(a, b, c, oa, ob, oc, va, vb, vc, sems):
    parts = 4
    step = a.shape[0] // parts
    moves = [(b, vb, ob), (c, vc, oc)]
    moves += [tuple(r.at[pl.ds(i * step, step), :] for r in (a, va, oa)) for i in range(parts)]
    ins = [pltpu.make_async_copy(r, v, sems.at[i]) for i, (r, v, o) in enumerate(moves)]
    outs = [pltpu.make_async_copy(v, o, sems.at[len(moves) + i]) for i, (r, v, o) in enumerate(moves)]
    for cpy in ins:
        cpy.start()
    for c_in, c_out in zip(ins, outs):
        c_in.wait()
        c_out.start()
    for cpy in outs:
        cpy.wait()


def local(
    hidden_in, norm_gain, seq_lengths, w_query, b_query, w_key, b_key, w_value, b_value, w_out
):
    T, D1 = hidden_in.shape
    D = w_query.shape[0]
    H1 = w_query.shape[1]
    NH = H1 // HD
    f = (ROPE_BASE ** (-np.arange(HD // 2) / (HD // 2))).astype(np.float32)
    freq = jnp.asarray(np.concatenate([f, f]).reshape(1, HD))
    vm = pl.BlockSpec(memory_space=pltpu.VMEM)
    hb = pl.BlockSpec(memory_space=pl.ANY)
    V = pltpu.VMEM
    made = pl.pallas_call(
        kernel,
        out_shape=(
            jax.ShapeDtypeStruct((T, D1), BF),
            jax.ShapeDtypeStruct((T, HD), BF),
            jax.ShapeDtypeStruct((T, HD), BF),
        ),
        in_specs=[hb] * 11,
        out_specs=(hb, hb, hb),
        scratch_shapes=[
            V((1, D), F32), V((NH, HD), BF), V((1, HD), BF), V((1, HD), BF), V((1, HD), F32),
            pltpu.SMEM(seq_lengths.shape, jnp.int32),
            V((T, D), BF), V((T, D), BF), V((D, H1 + 2 * HD), BF), V(w_out.shape, BF),
            V((32, T, HD), BF), V((32, T, HD), BF), V((T, 8 * H1), BF), V((NH, T, HD), BF),
            V((NH, T, HD), F32), V((NH, T, HD), F32), V((NH, T, HD), F32),
            V((T, HD), F32), V((T, HD), F32), V((T, HD), BF), V((32, T, HD), BF), V((T, HD), F32),
            V((T, D1), F32), V((T, D1), BF),
            pltpu.SemaphoreType.DMA((21,)),
            pltpu.SemaphoreType.DMA((28,)), pltpu.SemaphoreType.DMA((32,)),
            pltpu.SemaphoreType.DMA((28,)), pltpu.SemaphoreType.DMA((32,)),
            pltpu.SemaphoreType.DMA((SENDS,)), pltpu.SemaphoreType.DMA((64,)),
        ],
        compiler_params=pltpu.CompilerParams(
            collective_id=0, has_side_effects=True, vmem_limit_bytes=60 * 1024 * 1024
        ),
        name="layer",
    )(
        hidden_in, norm_gain.reshape(1, D), seq_lengths, w_query, b_query.reshape(NH, HD),
        w_key, b_key.reshape(1, HD), w_value, b_value.reshape(1, HD), w_out, freq,
    )
    return pl.pallas_call(
        finish,
        out_shape=tuple(jax.ShapeDtypeStruct(m.shape, m.dtype) for m in made),
        in_specs=[hb, hb, hb],
        out_specs=(hb, hb, hb),
        scratch_shapes=[V(m.shape, m.dtype) for m in made] + [pltpu.SemaphoreType.DMA((12,))],
        name="finish",
    )(*made)


def solution(mesh):
    placed = (
        P("cp", "tp"), P(), P(), P(None, "tp"), P("tp"), P(None, "tp"), P("tp"),
        P(None, "tp"), P("tp"), P(None, "tp"),
    )
    return jax.shard_map(
        local, mesh=mesh, in_specs=placed,
        out_specs=(P("cp", "tp"), P("cp", "tp"), P("cp", "tp")), check_vma=False,
    )
```
